32 devices in a mesh: rep: 4 (over z), fsdp: 8 (over y, x, core).
Axes of the slice: x: 2, y: 2, z: 4, core: 2. Of those that a mesh axis runs over, the one named last changes fastest.
Arguments:
- hidden_in: float32 [32768, 384], P(('rep', 'fsdp')), may hold values from -6 to 6
- cotangent: float32 [32768, 384], P(('rep', 'fsdp')), may hold values from -6 to 6
- segment_ids: int32 [32768], P(('rep', 'fsdp')), may hold values from -1 to 4, as said below
- norm1_gain: bfloat16 [2, 384], P(None, 'fsdp'), may hold values from 0.5 to 1.5
- norm1_bias: bfloat16 [2, 384], P(None, 'fsdp'), may hold values from -3 to 3
- qkv_weight: bfloat16 [2, 384, 1152], P(None, 'fsdp'), may hold values from -0.3125 to 0.3125
- query_bias: bfloat16 [2, 384], P(None, 'fsdp'), may hold values from -3 to 3
- value_bias: bfloat16 [2, 384], P(None, 'fsdp'), may hold values from -3 to 3
- out_weight: bfloat16 [2, 384, 384], P(None, 'fsdp'), may hold values from -1.25 to 1.25
- out_bias: bfloat16 [2, 384], P(None, 'fsdp'), may hold values from -3 to 3
- norm2_gain: bfloat16 [2, 384], P(None, 'fsdp'), may hold values from 0.5 to 1.5
- norm2_bias: bfloat16 [2, 384], P(None, 'fsdp'), may hold values from -3 to 3
- up_weight: bfloat16 [2, 384, 1536], P(None, 'fsdp'), may hold values from -0.3125 to 0.3125
- up_bias: bfloat16 [2, 1536], P(None, 'fsdp'), may hold values from -3 to 3
- down_weight: bfloat16 [2, 1536, 384], P(None, 'fsdp'), may hold values from -0.15625 to 0.15625
- down_bias: bfloat16 [2, 384], P(None, 'fsdp'), may hold values from -3 to 3
Outputs:
- output: float32 [32768, 384], P(('rep', 'fsdp'))
- grad_input: float32 [32768, 384], P(('rep', 'fsdp'))
- grad_norm1_gain: float32 [2, 384], P(None, 'fsdp')
- grad_norm1_bias: float32 [2, 384], P(None, 'fsdp')
- grad_qkv_weight: float32 [2, 384, 1152], P(None, 'fsdp')
- grad_query_bias: float32 [2, 384], P(None, 'fsdp')
- grad_value_bias: float32 [2, 384], P(None, 'fsdp')
- grad_out_weight: float32 [2, 384, 384], P(None, 'fsdp')
- grad_out_bias: float32 [2, 384], P(None, 'fsdp')
- grad_norm2_gain: float32 [2, 384], P(None, 'fsdp')
- grad_norm2_bias: float32 [2, 384], P(None, 'fsdp')
- grad_up_weight: float32 [2, 384, 1536], P(None, 'fsdp')
- grad_up_bias: float32 [2, 1536], P(None, 'fsdp')
- grad_down_weight: float32 [2, 1536, 384], P(None, 'fsdp')
- grad_down_bias: float32 [2, 384], P(None, 'fsdp')
The draws below stay inside these ranges and needn't reach their ends.
Inputs may be any that keep to these rules, and one draw needn't show every extreme that they name: `segment_ids`: in each aligned block of 1024 slots, images of 197 tokens are numbered 0, 1, 2 ... from the block's start, each whole and contiguous, followed by -1 in all remaining slots; a block holds 2 to 5 images, and some block holds 5.
All inputs are finite; a program needn't handle non-finite values.
Results may differ from the reference program's by a relative error of at most 0.012.
Values may be sent and summed in bfloat16 or wider, within the bound.
A program may use at most 256 MiB of HBM per device.

```python
import jax
import jax.numpy as jnp
from jax import lax

D = 384
HEADS = 6
HEAD_DIM = 64
FF = 1536
IMG = 197
LAYERS = 2
ROWS = 1024
TOKENS = 32768


def draw_segment_ids(key, part):
    blocks = TOKENS // ROWS
    most_images = ROWS // IMG
    counts = jax.random.randint(key, (blocks,), 2, most_images + 1)
    counts = jnp.where(jnp.arange(blocks) == 0, most_images, counts)
    slots = jnp.arange(TOKENS)
    image_num = slots % ROWS // IMG
    block_num = slots // ROWS
    return jnp.where(image_num < counts[block_num], image_num, -1).astype(jnp.int32)


def level_of(own_key, extent, split, least, high):
    level, own = 1.0, jax.random.fold_in(own_key, 6)
    for dim, shards_of in split:
        heights = jnp.exp(jax.random.uniform(jax.random.fold_in(own, dim), (shards_of,), jnp.float32, least / len(split), high / len(split)))
        level = level * jnp.repeat(heights, extent[dim] // shards_of).reshape([-1 if axis == dim else 1 for axis in range(len(extent))])
    return level


def centred(stream_key, shape, deviation, bound, cuts=(), dtype=jnp.bfloat16):
    factor_of = level_of(stream_key, shape, cuts, -0.22, 0.18) if cuts else 1.0
    array = jax.random.normal(stream_key, shape, jnp.float32) * deviation * factor_of
    return jnp.minimum(jnp.maximum(array, -bound), bound).astype(dtype)


def setup_inputs(seed: int = 0) -> dict:
    key_list = jax.random.split(jax.random.key(seed), 17)
    return {
        "hidden_in": centred(key_list[0], (TOKENS, D), 1.0, 6.0, ((0, 32),), jnp.float32),
        "cotangent": centred(key_list[1], (TOKENS, D), 1.0, 6.0, ((0, 32),), jnp.float32),
        "segment_ids": draw_segment_ids(jax.random.fold_in(key_list[16], 71), 0),
        "norm1_gain": jnp.clip(1.0 + 0.1 * jax.random.normal(key_list[3], (LAYERS, D), jnp.float32), 0.5, 1.5).astype(jnp.bfloat16),
        "norm1_bias": centred(key_list[4], (LAYERS, D), 0.5, 3.0, ((1, 8),)),
        "qkv_weight": centred(key_list[5], (LAYERS, D, 3 * D), D ** -0.5, 0.3125, ((1, 8),)),
        "query_bias": centred(key_list[6], (LAYERS, D), 0.5, 3.0, ((1, 8),)),
        "value_bias": centred(key_list[7], (LAYERS, D), 0.5, 3.0, ((1, 8),)),
        "out_weight": centred(key_list[8], (LAYERS, D, D), (D // 16) ** -0.5, 1.25, ((1, 8),)),
        "out_bias": centred(key_list[9], (LAYERS, D), 0.5, 3.0, ((1, 8),)),
        "norm2_gain": jnp.clip(1.0 + 0.1 * jax.random.normal(key_list[10], (LAYERS, D), jnp.float32), 0.5, 1.5).astype(jnp.bfloat16),
        "norm2_bias": centred(key_list[11], (LAYERS, D), 0.5, 3.0, ((1, 8),)),
        "up_weight": centred(key_list[12], (LAYERS, D, FF), D ** -0.5, 0.3125, ((1, 8),)),
        "up_bias": centred(key_list[13], (LAYERS, FF), 0.5, 3.0, ((1, 8),)),
        "down_weight": centred(key_list[14], (LAYERS, FF, D), FF ** -0.5, 0.15625, ((1, 8),)),
        "down_bias": centred(key_list[15], (LAYERS, D), 0.5, 3.0, ((1, 8),)),
    }


norm_eps = 1e-06
neg_fill = -1e+30
root_half = 0.7071067811865476
inv_root_tau = 0.3989422804014327

def norm_forward(stream, gain_vec, bias_vec):
    center = stream - lax.optimization_barrier(jnp.mean(stream, -1, keepdims=True))
    recip = lax.rsqrt(lax.optimization_barrier(jnp.mean(center * center, -1, keepdims=True)) + norm_eps)
    normed = center * recip
    return (normed * gain_vec.astype(jnp.float32) + bias_vec.astype(jnp.float32), normed, recip)

def norm_backward(grad_norm, normed, recip, gain_vec):
    scaled = grad_norm * gain_vec.astype(jnp.float32)
    grad_stream = recip * (scaled - lax.optimization_barrier(jnp.mean(scaled, -1, keepdims=True)) - normed * lax.optimization_barrier(jnp.mean(scaled * normed, -1, keepdims=True)))
    return (grad_stream, lax.optimization_barrier(jnp.sum(grad_norm * normed, 0)), lax.optimization_barrier(jnp.sum(grad_norm, 0)))

def gelu_value(pre_act):
    return 0.5 * pre_act * (1.0 + lax.erf(pre_act * root_half))

def gelu_slope(pre_act):
    return 0.5 * (1.0 + lax.erf(pre_act * root_half)) + pre_act * jnp.exp(-0.5 * pre_act * pre_act) * inv_root_tau

def matmul(left, right):
    return jnp.dot(left, right, preferred_element_type=jnp.float32)

def split_heads(rows_arr):
    return rows_arr.reshape(rows_arr.shape[0], HEADS, HEAD_DIM)

def masked_scores(query_blk, key_all, seg_blk, seg_all):
    scores = jnp.einsum('qhd,khd->hqk', query_blk.astype(jnp.float32), key_all.astype(jnp.float32))
    same_image = seg_blk[:, None] == seg_all[None, :]
    return jnp.where(same_image[None], scores, neg_fill)

def attend_forward(query_all, key_all, value_all, seg_all):
    count = query_all.shape[0]
    block = min(512, count)
    query3 = split_heads(query_all)
    key3 = split_heads(key_all)
    value3 = split_heads(value_all)
    pieces = []
    totals = []
    for start in range(0, count, block):
        scores = masked_scores(query3[start:start + block], key3, seg_all[start:start + block], seg_all)
        top_score = lax.optimization_barrier(jnp.max(scores, -1, keepdims=True))
        expo = jnp.exp(scores - top_score)
        denom = lax.optimization_barrier(jnp.sum(expo, -1, keepdims=True))
        probs_low = (expo / denom).astype(jnp.bfloat16)
        mixed = jnp.einsum('hqk,khd->qhd', probs_low.astype(jnp.float32), value3.astype(jnp.float32))
        pieces.append(mixed.reshape(block, -1).astype(jnp.bfloat16))
        totals.append((top_score + jnp.log(denom))[:, :, 0])
    return (jnp.concatenate(pieces, 0), jnp.concatenate(totals, 1))

def attend_backward(query_all, key_all, value_all, seg_all, log_total, grad_mixed):
    count = query_all.shape[0]
    block = min(512, count)
    query3 = split_heads(query_all).astype(jnp.float32)
    key3 = split_heads(key_all).astype(jnp.float32)
    value3 = split_heads(value_all).astype(jnp.float32)
    grad3 = split_heads(grad_mixed).astype(jnp.float32)
    grad_key = jnp.zeros((count, HEADS, HEAD_DIM), jnp.float32)
    grad_value = jnp.zeros((count, HEADS, HEAD_DIM), jnp.float32)
    grad_query = []
    for start in range(0, count, block):
        scores = masked_scores(query3[start:start + block], key3, seg_all[start:start + block], seg_all)
        probs = jnp.exp(scores - log_total[:, start:start + block, None])
        probs_low = probs.astype(jnp.bfloat16).astype(jnp.float32)
        grad_blk = grad3[start:start + block]
        grad_probs = jnp.einsum('qhd,khd->hqk', grad_blk, value3)
        delta = lax.optimization_barrier(jnp.sum(probs * grad_probs, -1, keepdims=True))
        grad_scores = (probs * (grad_probs - delta)).astype(jnp.bfloat16).astype(jnp.float32)
        grad_query.append(jnp.einsum('hqk,khd->qhd', grad_scores, key3).reshape(block, -1))
        grad_key = grad_key + jnp.einsum('hqk,qhd->khd', grad_scores, query3[start:start + block])
        grad_value = grad_value + jnp.einsum('hqk,qhd->khd', probs_low, grad_blk)
    return (jnp.concatenate(grad_query, 0), grad_key.reshape(count, -1), grad_value.reshape(count, -1))

def layer_forward(stream, seg_all, params):
    norm1_gain, norm1_bias, qkv_weight, query_bias, value_bias, out_weight, out_bias, norm2_gain, norm2_bias, up_weight, up_bias, down_weight, down_bias = params
    width = stream.shape[1]
    scale = HEAD_DIM ** (-0.5)
    normed_a = norm_forward(stream, norm1_gain, norm1_bias)[0].astype(jnp.bfloat16)
    proj = matmul(normed_a, qkv_weight)
    query = ((proj[:, :width] + query_bias.astype(jnp.float32)) * scale).astype(jnp.bfloat16)
    key_rows = proj[:, width:2 * width].astype(jnp.bfloat16)
    value_rows = (proj[:, 2 * width:] + value_bias.astype(jnp.float32)).astype(jnp.bfloat16)
    attended, log_total = attend_forward(query, key_rows, value_rows, seg_all)
    stream_mid = stream + matmul(attended, out_weight) + out_bias.astype(jnp.float32)
    normed_m = norm_forward(stream_mid, norm2_gain, norm2_bias)[0].astype(jnp.bfloat16)
    pre_act = matmul(normed_m, up_weight) + up_bias.astype(jnp.float32)
    hidden = gelu_value(pre_act).astype(jnp.bfloat16)
    stream_out = stream_mid + matmul(hidden, down_weight) + down_bias.astype(jnp.float32)
    return (stream_out, (stream, normed_a, query, key_rows, value_rows, attended, log_total, stream_mid, normed_m, pre_act, hidden))

def layer_backward(grad_out, seg_all, params, saved):
    norm1_gain, norm1_bias, qkv_weight, query_bias, value_bias, out_weight, out_bias, norm2_gain, norm2_bias, up_weight, up_bias, down_weight, down_bias = params
    stream, normed_a, query, key_rows, value_rows, attended, log_total, stream_mid, normed_m, pre_act, hidden = saved
    scale = HEAD_DIM ** (-0.5)
    grad_out_low = grad_out.astype(jnp.bfloat16)
    grad_down_bias = lax.optimization_barrier(jnp.sum(grad_out, 0))
    grad_down_weight = matmul(hidden.T, grad_out_low)
    grad_pre = matmul(grad_out_low, down_weight.T) * gelu_slope(pre_act)
    grad_pre_low = grad_pre.astype(jnp.bfloat16)
    grad_up_bias = lax.optimization_barrier(jnp.sum(grad_pre, 0))
    grad_up_weight = matmul(normed_m.T, grad_pre_low)
    grad_m = matmul(grad_pre_low, up_weight.T)
    unused2, normed2, recip2 = norm_forward(stream_mid, norm2_gain, norm2_bias)
    grad_stream2, grad_norm2_gain, grad_norm2_bias = norm_backward(grad_m, normed2, recip2, norm2_gain)
    grad_mid = grad_out + grad_stream2
    grad_mid_low = grad_mid.astype(jnp.bfloat16)
    grad_out_bias = lax.optimization_barrier(jnp.sum(grad_mid, 0))
    grad_out_weight = matmul(attended.T, grad_mid_low)
    grad_attended = matmul(grad_mid_low, out_weight.T).astype(jnp.bfloat16)
    grad_query, grad_key, grad_value = attend_backward(query, key_rows, value_rows, seg_all, log_total, grad_attended)
    grad_query = grad_query * scale
    grad_proj = jnp.concatenate([grad_query, grad_key, grad_value], 1).astype(jnp.bfloat16)
    grad_query_bias = lax.optimization_barrier(jnp.sum(grad_query, 0))
    grad_value_bias = lax.optimization_barrier(jnp.sum(grad_value, 0))
    grad_qkv_weight = matmul(normed_a.T, grad_proj)
    grad_a = matmul(grad_proj, qkv_weight.T)
    unused1, normed1, recip1 = norm_forward(stream, norm1_gain, norm1_bias)
    grad_stream1, grad_norm1_gain, grad_norm1_bias = norm_backward(grad_a, normed1, recip1, norm1_gain)
    grads = (grad_norm1_gain, grad_norm1_bias, grad_qkv_weight, grad_query_bias, grad_value_bias, grad_out_weight, grad_out_bias, grad_norm2_gain, grad_norm2_bias, grad_up_weight, grad_up_bias, grad_down_weight, grad_down_bias)
    return (grad_mid + grad_stream1, grads)

def block_pass(stream_blk, cotan_blk, seg_blk, params):
    stream = stream_blk
    saves = []
    for layer_idx in range(LAYERS):
        layer_params = tuple((entry[layer_idx] for entry in params))
        stream, saved = layer_forward(stream, seg_blk, layer_params)
        saves.append(saved)
    grad_now = cotan_blk * (seg_blk >= 0).astype(jnp.float32)[:, None]
    layer_grads = [None] * LAYERS
    for layer_idx in range(LAYERS - 1, -1, -1):
        layer_params = tuple((entry[layer_idx] for entry in params))
        grad_now, layer_grads[layer_idx] = layer_backward(grad_now, seg_blk, layer_params, saves[layer_idx])
    stacked = tuple((jnp.stack([layer_grads[idx][field] for idx in range(LAYERS)], 0) for field in range(13)))
    return (stream, grad_now, stacked)

def reference(hidden_in, cotangent, segment_ids, norm1_gain, norm1_bias, qkv_weight, query_bias, value_bias, out_weight, out_bias, norm2_gain, norm2_bias, up_weight, up_bias, down_weight, down_bias):
    params = (norm1_gain, norm1_bias, qkv_weight, query_bias, value_bias, out_weight, out_bias, norm2_gain, norm2_bias, up_weight, up_bias, down_weight, down_bias)
    width = hidden_in.shape[1]
    count_blocks = hidden_in.shape[0] // ROWS
    inputs = (hidden_in.reshape(count_blocks, ROWS, width), cotangent.reshape(count_blocks, ROWS, width), segment_ids.reshape(count_blocks, ROWS))
    start_sums = tuple((jnp.zeros(entry.shape, jnp.float32) for entry in params))

    def scan_step(carry, item):
        out_blk, grad_blk, grads = block_pass(item[0], item[1], item[2], params)
        return (tuple((total + part for total, part in zip(carry, grads))), (out_blk, grad_blk))
    totals, results = lax.scan(scan_step, start_sums, inputs)
    return (results[0].reshape(-1, width), results[1].reshape(-1, width), totals[0], totals[1], totals[2], totals[3], totals[4], totals[5], totals[6], totals[7], totals[8], totals[9], totals[10], totals[11], totals[12])
```

```python
import functools
from types import SimpleNamespace as NS
import jax
import jax.numpy as jnp
from jax import lax
from jax.experimental import pallas as pl
from jax.experimental.pallas import tpu as pltpu

HEADS = 6
HEAD_DIM = 64
IMG = 197
STEP = 192
QWIN = 224
KWIN = 256
TILE = 256
norm_eps = 1e-06
neg_fill = -1e30
root_half = 0.7071067811865476
inv_root_tau = 0.3989422804014327
F32, BF16 = jnp.float32, jnp.bfloat16


def nn(a, b):
    return lax.dot_general(a, b, (((1,), (0,)), ((), ())), preferred_element_type=F32)


def nt(a, b):
    return lax.dot_general(a, b, (((1,), (1,)), ((), ())), preferred_element_type=F32)


def tn(a, b):
    return lax.dot_general(a, b, (((0,), (0,)), ((), ())), preferred_element_type=F32)


def fold8(x):
    return jnp.sum(x.reshape(x.shape[0] // 8, 8, x.shape[1]), axis=0)


def norm(x):
    c = x - jnp.mean(x, -1, keepdims=True)
    r = lax.rsqrt(jnp.mean(c * c, -1, keepdims=True) + norm_eps)
    return c * r, r


def norm_back(grad, n, r, gain):
    e = grad * gain
    return r * (e - jnp.mean(e, -1, keepdims=True) - n * jnp.mean(e * n, -1, keepdims=True))


def gelu_both(pre):
    cdf = 0.5 * (1.0 + lax.erf(pre * root_half))
    return pre * cdf, cdf + pre * jnp.exp(-0.5 * pre * pre) * inv_root_tau


def vrow(R, l, k):
    return R.vec[12 * l + k : 12 * l + k + 1, :]


def add_sum(R, l, k, x):
    R.vacc[12 * l + k] += fold8(x)


def stage_qkv(R, l, src):
    gain, bias, qb, vb = (vrow(R, l, k) for k in range(4))

    def tile(i, c):
        rows = pl.ds(pl.multiple_of(i * TILE, TILE), TILE)
        n, r = norm(src[rows, :])
        R.n1[l, rows, :] = n
        R.stats[l, rows, 0:1] = r
        a = (n * gain + bias).astype(BF16)
        R.aT[l, :, rows] = a.T
        proj = nn(a, R.wqkv[l])
        R.q[l, rows, :] = ((proj[:, :384] + qb) * (HEAD_DIM**-0.5)).astype(BF16)
        R.k[l, rows, :] = proj[:, 384:768].astype(BF16)
        R.v[l, rows, :] = (proj[:, 768:] + vb).astype(BF16)
        return c

    lax.fori_loop(0, R.rows // TILE, tile, 0)


def stack_heads(x, low):
    zero = jnp.zeros_like(x)
    return jnp.concatenate([jnp.where(low, x, zero), jnp.where(low, zero, x)], 0)


def attend(q, k, v, bias):
    n = q.shape[0]
    low = lax.broadcasted_iota(jnp.int32, (1, 128), 1) < HEAD_DIM
    s = nt(stack_heads(q, low), k)
    if bias.shape[0] == n:
        bias = jnp.concatenate([bias, bias], 0)
    s = s + bias
    top = jnp.max(s, -1, keepdims=True)
    p = jnp.exp(s - top)
    den = jnp.sum(p, -1, keepdims=True)
    o = nn((p * (1.0 / den)).astype(BF16), v)
    return jnp.where(low, o[:n], o[n:]).astype(BF16), top + jnp.log(den)


def stage_attend(R, l):
    def put(pr, start, first, o, lse):
        n = o.shape[0]
        lanes = slice(128 * pr, 128 * pr + 128)
        head = pl.ds(start, 32)
        rest = pl.ds(start + 32, n - 32)
        old = start + lax.broadcasted_iota(jnp.int32, (32, 1), 0) < first
        R.att[head, lanes] = jnp.where(old, R.att[head, lanes].astype(F32), o[:32].astype(F32)).astype(BF16)
        R.att[rest, lanes] = o[32:]
        for h in range(2):
            col = slice(2 + 2 * pr + h, 3 + 2 * pr + h)
            R.stats[l, head, col] = jnp.where(old, R.stats[l, head, col], lse[n * h : n * h + 32])
            R.stats[l, rest, col] = lse[n * h + 32 : n * h + n]

    def window(j, c):
        start = pl.multiple_of(j * STEP, STEP)
        col = lax.broadcasted_iota(jnp.int32, (1, KWIN), 1)
        bias = jnp.where((col >= 5 * j) & (col < 5 * j + IMG), 0.0, neg_fill)
        for pr in range(3):
            lanes = slice(128 * pr, 128 * pr + 128)
            o, lse = attend(
                R.q[l, pl.ds(start, QWIN), lanes], R.k[l, pl.ds(start, KWIN), lanes],
                R.v[l, pl.ds(start, KWIN), lanes], bias)
            put(pr, start, IMG * j, o, lse)
        return c

    lax.fori_loop(0, 2, window, 0)

    def rest(t, c):
        start = pl.multiple_of(2 * STEP + t * 128, 128)
        bias = R.segbias[pl.ds(pl.multiple_of(t * 128, 128), 128), :]
        for pr in range(3):
            lanes = slice(128 * pr, 128 * pr + 128)
            o, lse = attend(
                R.q[l, pl.ds(start, 128), lanes], R.k[l, 2 * STEP :, lanes],
                R.v[l, 2 * STEP :, lanes], bias)
            put(pr, start, 2 * IMG, o, lse)
        return c

    lax.fori_loop(0, (R.rows - 2 * STEP) // 128, rest, 0)


def stage_mlp(R, l, src, dst):
    ob, gain, bias, db = (vrow(R, l, k) for k in (4, 5, 6, 7))

    def tile(i, c):
        rows = pl.ds(pl.multiple_of(i * TILE, TILE), TILE)
        att = R.att[rows, :]
        R.attT[l, :, rows] = att.T
        mid = src[rows, :] + nn(att, R.wo[l]) + ob
        n, r = norm(mid)
        R.n2[l, rows, :] = n
        R.stats[l, rows, 1:2] = r
        m = (n * gain + bias).astype(BF16)
        R.mT[l, :, rows] = m.T
        acc = mid + db
        for ch in range(4):
            cols = slice(384 * ch, 384 * ch + 384)
            pre = nn(m, R.wup[l, :, cols]) + vrow(R, l, 8 + ch)
            hid, slope = gelu_both(pre)
            hid = hid.astype(BF16)
            R.hidT[l, cols, rows] = hid.T
            R.slope[l, rows, cols] = slope.astype(BF16)
            acc = acc + nn(hid, R.wd[l, cols, :])
        dst[rows, :] = acc
        return c

    lax.fori_loop(0, R.rows // TILE, tile, 0)


def stage_mlp_back(R, l):
    gain = vrow(R, l, 5)

    def tile(i, c):
        rows = pl.ds(pl.multiple_of(i * TILE, TILE), TILE)
        g = R.g[rows, :]
        gl = g.astype(BF16)
        R.gl[rows, :] = gl
        add_sum(R, l, 7, g)
        dm = jnp.zeros_like(g)
        for ch in range(4):
            cols = slice(384 * ch, 384 * ch + 384)
            dpre = nt(gl, R.wd[l, cols, :]) * R.slope[l, rows, cols].astype(F32)
            add_sum(R, l, 8 + ch, dpre)
            dpre = dpre.astype(BF16)
            R.slope[l, rows, cols] = dpre
            dm = dm + nt(dpre, R.wup[l, :, cols])
        n = R.n2[l, rows, :]
        add_sum(R, l, 5, dm * n)
        add_sum(R, l, 6, dm)
        gm = g + norm_back(dm, n, R.stats[l, rows, 1:2], gain)
        add_sum(R, l, 4, gm)
        R.g[rows, :] = gm
        gml = gm.astype(BF16)
        R.gml[rows, :] = gml
        R.datt[rows, :] = nt(gml, R.wo[l]).astype(BF16)
        return c

    lax.fori_loop(0, R.rows // TILE, tile, 0)


def stage_weight_down(R, l):
    def block(b, c):
        rows = pl.ds(pl.multiple_of(b * n, n), n)
        R.grad(0, l)[lax.rem(b, 2), b // 2] = nn(R.hidT[l, rows, :], R.gl[...]).astype(BF16)
        return c

    n = R.hidT.shape[1] // 8
    lax.fori_loop(0, 8, block, 0)


def put_rows(ref, cols, x):
    n = x.shape[0] // 8
    for b in range(8):
        ref[b % 2, b // 2, :, cols] = x[n * b : n * b + n].astype(BF16)


def stage_weight_up(R, l):
    def block(b, c):
        cols = pl.ds(pl.multiple_of(b * 256, 256), 256)
        put_rows(R.grad(1, l), cols, nn(R.mT[l], R.slope[l, :, cols]))
        return c

    lax.fori_loop(0, 6, block, 0)


def stage_weight_out(R, l):
    put_rows(R.grad(2, l), slice(1152, 1536), nn(R.attT[l], R.gml[...]))


def stage_weight_qkv(R, l):
    def block(b, c):
        cols = pl.ds(pl.multiple_of(b * 384, 128), 384)
        put_rows(R.grad(2, l), cols, nn(R.aT[l], R.dproj[:, cols]))
        return c

    lax.fori_loop(0, 3, block, 0)


def stage_attend_back(R, l):
    R.dproj[...] = jnp.zeros(R.dproj.shape, BF16)
    low = lax.broadcasted_iota(jnp.int32, (1, 128), 1) < HEAD_DIM

    def put(start, col, x):
        n = x.shape[0]
        head = pl.ds(start, 32)
        lanes = slice(col, col + 128)
        R.dproj[head, lanes] = (R.dproj[head, lanes].astype(F32) + x[:32]).astype(BF16)
        R.dproj[pl.ds(start + 32, n - 32), lanes] = x[32:].astype(BF16)

    def window(j, c):
        start = pl.multiple_of(j * STEP, STEP)
        qrows, krows = pl.ds(start, QWIN), pl.ds(start, KWIN)
        col = lax.broadcasted_iota(jnp.int32, (1, KWIN), 1)
        colbias = jnp.where((col >= 5 * j) & (col < 5 * j + IMG), 0.0, neg_fill)
        row = lax.broadcasted_iota(jnp.int32, (QWIN, 1), 0)
        rowin = (row >= 5 * j) & (row < 5 * j + IMG)
        for pr in range(3):
            lanes = slice(128 * pr, 128 * pr + 128)
            q01 = stack_heads(R.q[l, qrows, lanes], low)
            do01 = stack_heads(R.datt[qrows, lanes], low)
            k, v = R.k[l, krows, lanes], R.v[l, krows, lanes]
            lse01 = jnp.concatenate(
                [jnp.where(rowin, R.stats[l, qrows, c : c + 1], -neg_fill) for c in (2 + 2 * pr, 3 + 2 * pr)], 0)
            p = jnp.exp((nt(q01, k) - lse01) + colbias)
            pdp = nt(do01, v)
            delta = jnp.sum(p * pdp, -1, keepdims=True)
            ds = (p * (pdp - delta)).astype(BF16)
            dq01 = nn(ds, k)
            dq = jnp.where(low, dq01[:QWIN], dq01[QWIN:]) * (HEAD_DIM**-0.5)
            dk = tn(ds, q01)[:QWIN]
            dv = tn(p.astype(BF16), do01)[:QWIN]
            put(start, 128 * pr, dq)
            put(start, 384 + 128 * pr, dk)
            put(start, 768 + 128 * pr, dv)
            R.vacc[12 * l + 2, :, lanes] += fold8(dq)
            R.vacc[12 * l + 3, :, lanes] += fold8(dv)
        return c

    lax.fori_loop(0, 5, window, 0)


def stage_qkv_back(R, l):
    gain = vrow(R, l, 0)

    def tile(i, c):
        rows = pl.ds(pl.multiple_of(i * TILE, TILE), TILE)
        da = nt(R.dproj[rows, :], R.wqkv[l])
        n = R.n1[l, rows, :]
        add_sum(R, l, 0, da * n)
        add_sum(R, l, 1, da)
        R.g[rows, :] = R.g[rows, :] + norm_back(da, n, R.stats[l, rows, 0:1], gain)
        return c

    lax.fori_loop(0, R.rows // TILE, tile, 0)


def stage_segments(R):
    seg = R.seg[...].astype(F32)
    cols = jnp.broadcast_to(seg, (128, R.rows)).T
    R.segcol[...] = cols
    keys = seg[:, 2 * STEP :]

    def tile(t, c):
        rows = pl.ds(pl.multiple_of(t * 128, 128), 128)
        mine = R.segcol[pl.ds(pl.multiple_of(2 * STEP + t * 128, 128), 128), :1]
        R.segbias[rows, :] = jnp.where(mine == keys, 0.0, neg_fill)
        return c

    lax.fori_loop(0, (R.rows - 2 * STEP) // 128, tile, 0)


def stage_cotangent(R):
    def tile(i, c):
        rows = pl.ds(pl.multiple_of(i * TILE, TILE), TILE)
        R.g[rows, :] = jnp.where(R.segcol[rows, :1] >= 0.0, R.cot[rows, :], 0.0)
        return c

    lax.fori_loop(0, R.rows // TILE, tile, 0)


def compute(R, streams, hook):
    R.vacc[...] = jnp.zeros(R.vacc.shape, F32)
    stage_segments(R)
    for l in range(2):
        hook("qkv", l)
        stage_qkv(R, l, streams[l])
        hook("att", l)
        stage_attend(R, l)
        hook("mlp", l)
        stage_mlp(R, l, streams[l], streams[l + 1])
    hook("fwd", 0)
    stage_cotangent(R)
    for l in (1, 0):
        stage_mlp_back(R, l)
        hook("b0", l)
        stage_weight_down(R, l)
        hook("dD", l)
        stage_weight_up(R, l)
        hook("dU", l)
        stage_weight_out(R, l)
        hook("dO", l)
        stage_attend_back(R, l)
        hook("batt", l)
        stage_weight_qkv(R, l)
        hook("dA", l)
        stage_qkv_back(R, l)
        hook("b1", l)


MESH = pl.DeviceIdType.MESH
VECTORS = 8


def scratch_single(rows, d, f):
    v = pltpu.VMEM
    return dict(
        mid=v((rows, d), F32), n1=v((2, rows, d), F32), n2=v((2, rows, d), F32),
        stats=v((2, rows, 128), F32), aT=v((2, d, rows), BF16),
        q=v((2, rows, d), BF16), k=v((2, rows, d), BF16), v=v((2, rows, d), BF16),
        att=v((rows, d), BF16), attT=v((2, d, rows), BF16), mT=v((2, d, rows), BF16),
        hidT=v((2, f, rows), BF16), slope=v((2, rows, f), BF16),
        segcol=v((rows, 128), F32), segbias=v((rows - 2 * STEP, rows - 2 * STEP), F32),
        gl=v((rows, d), BF16), gml=v((rows, d), BF16),
        dproj=v((rows, 3 * d), BF16), vacc=v((24, 8, d), F32),
    )


def scratch_comm(d, f):
    v, dma = pltpu.VMEM, pltpu.SemaphoreType.DMA
    s, t = d // 8, f // 8
    return dict(
        wqkv=v((2, d, 3 * d), BF16), wo=v((2, d, d), BF16), wup=v((2, d, f), BF16), wd=v((2, f, d), BF16),
        pk=v((24, 128), F32), mine=v((24, d), F32), gat=v((8, 24, d), F32), vec=v((24, d), F32),
        dD=v((2, 4, t, d), BF16), dU=v((2, 4, s, f), BF16), dA=v((2, 4, s, f), BF16),
        pD=v((2, 4, t, d), BF16), pU=v((2, 4, s, f), BF16), pA=v((2, 4, s, f), BF16),
        xD=v((2, 3, t, d), BF16), xU=v((2, 3, s, f), BF16), xA=v((2, 3, s, f), BF16),
        zb=v((6, 4, s, d), BF16), zr=v((6, 4, s, d), BF16),
        v0=v((2, 12, d), F32), v1=v((2, 12, d), F32), v2=v((2, 12, d), F32), v3=v((2, 3, 12, d), F32), v4=v((2, 4, 12, d), F32),
        loc=dma((9,)), ags=dma((9, 7)), agr=dma((9, 7)), s1s=dma((8,)), s1r=dma((8,)), s2s=dma((8, 3)), s2r=dma((8, 3)),
        s3s=dma((8, 3)), s3r=dma((8, 3)), s4s=dma((6, 3)), s4r=dma((6, 3)),
    )


class Comm:
    def __init__(self, R):
        self.R = R
        self.f = lax.axis_index("fsdp")
        self.z = lax.axis_index("rep")
        f = self.f
        self.c = lax.rem(f, 2)
        self.p = f // 2
        dx = 1 - 2 * lax.rem(self.p, 2)
        dy = 2 - 4 * (self.p // 2)
        self.chip = (self.p, self.p + dx, self.p + dy, self.p + dx + dy)
        self.core = 1 - self.c
        self.open, self.first = [], {}

    def dev(self, chip, core):
        return {"fsdp": 2 * chip + core}

    def rep(self, d):
        return lax.rem(self.z + d, 4)

    def push(self, src, dst, ss, rs, dev, keep=True):
        cp = pltpu.make_async_remote_copy(src, dst, ss, rs, device_id=dev, device_id_type=MESH)
        cp.start()
        if keep:
            self.open.append(cp)
        return cp

    def arrive(self, dst, ss, rs, dev):
        pltpu.make_async_remote_copy(dst, dst, ss, rs, device_id=dev, device_id_type=MESH).wait_recv()

    def barrier(self):
        bar = pltpu.get_barrier_semaphore()
        for dev in self.peers():
            pl.semaphore_signal(bar, inc=1, device_id=dev, device_id_type=MESH)
        pl.semaphore_wait(bar, 7)

    def peers(self):
        out = [self.dev(self.p, self.core)]
        out += [self.dev(self.chip[k], self.c) for k in (1, 2, 3)]
        out += [{"rep": self.rep(d)} for d in (1, 2, 3)]
        return out

    def slot(self, i, f):
        R = self.R
        if i == 0:
            return R.gat.at[f]
        l, k = (i - 1) // 4, (i - 1) % 4
        ref = (R.wqkv, R.wo, R.wup, R.wd)[k]
        n = ref.shape[1] // 8
        return ref.at[l, pl.ds(pl.multiple_of(f * n, n), n)]

    def source(self, i):
        R = self.R
        if i == 0:
            return R.mine
        l, k = (i - 1) // 4, (i - 1) % 4
        return (R.sqkv, R.so, R.sup, R.sd)[k].at[l]

    def gather_start(self, i):
        R, src, dst = self.R, self.source(i), self.slot(i, self.f)
        self.push(src, dst, R.ags.at[i, 1], R.agr.at[i, 1], self.dev(self.chip[1], self.c))
        self.push(src, dst, R.ags.at[i, 2], R.agr.at[i, 2], self.dev(self.chip[2], self.c))
        self.push(src, dst, R.ags.at[i, 3], R.agr.at[i, 3], self.dev(self.chip[3], self.c))
        self.push(src, dst, R.ags.at[i, 0], R.agr.at[i, 0], self.dev(self.p, self.core))
        pltpu.make_async_copy(src, dst, R.loc.at[i]).start()

    def gather_forward(self, i):
        R = self.R
        for k in (1, 2, 3):
            own = self.slot(i, 2 * self.chip[k] + self.c)
            self.arrive(own, R.ags.at[i, k], R.agr.at[i, k], self.dev(self.chip[k], self.c))
            self.push(own, own, R.ags.at[i, 3 + k], R.agr.at[i, 3 + k], self.dev(self.p, self.core))

    def gather_finish(self, i):
        R = self.R
        pltpu.make_async_copy(self.source(i), self.slot(i, self.f), R.loc.at[i]).wait()
        for k in (0, 1, 2, 3):
            j = 0 if k == 0 else 3 + k
            dst = self.slot(i, 2 * self.chip[k] + self.core)
            self.arrive(dst, R.ags.at[i, j], R.agr.at[i, j], self.dev(self.p, self.core))

    def grads(self, t):
        R, l = self.R, t // 3
        d, p, x = ((R.dD, R.pD, R.xD), (R.dU, R.pU, R.xU), (R.dA, R.pA, R.xA))[t % 3]
        return d, p.at[l], x.at[l]

    def step1(self, t):
        R = self.R
        d, p, x = self.grads(t)
        self.first[t] = self.push(d.at[self.core], p, R.s1s.at[t], R.s1r.at[t], self.dev(self.p, self.core), False)

    def step2(self, t):
        R = self.R
        d, p, x = self.grads(t)
        self.first[t].wait()
        for k in (3, 1, 2, 0):
            ch = self.chip[k]
            p[ch] = (d[self.c, ch].astype(F32) + p[ch].astype(F32)).astype(BF16)
            if k:
                self.push(p.at[ch], x.at[k - 1], R.s2s.at[t, k - 1], R.s2r.at[t, k - 1], self.dev(ch, self.c))

    def step3(self, t):
        R = self.R
        d, p, x = self.grads(t)
        for k in (1, 2, 3):
            self.arrive(x.at[k - 1], R.s2s.at[t, k - 1], R.s2r.at[t, k - 1], self.dev(self.chip[k], self.c))
        s = R.zb.shape[2]
        w = R.zb.shape[3]
        for j in range(4):
            at = (slice(s * j, s * j + s), slice(None)) if t % 3 == 0 else (slice(None), slice(w * j, w * j + w))
            tot = p[(self.p, *at)].astype(F32)
            for k in range(3):
                tot = tot + x[(k, *at)].astype(F32)
            R.zb[t, j] = tot.astype(BF16)
        for e in (1, 2, 3):
            r = self.rep(e)
            self.push(R.zb.at[t, r], R.zr.at[t, self.z], R.s3s.at[t, e - 1], R.s3r.at[t, e - 1], {"rep": r})

    def step4(self, t):
        R = self.R
        tot = R.zb[t, self.z].astype(F32)
        for e in (1, 2, 3):
            r = self.rep(4 - e)
            self.arrive(R.zr.at[t, r], R.s3s.at[t, e - 1], R.s3r.at[t, e - 1], {"rep": r})
            tot = tot + R.zr[t, r].astype(F32)
        R.zout[t, self.z] = tot.astype(BF16)
        for e in (1, 2, 3):
            here = R.zout.at[t, self.z]
            self.push(here, here, R.s4s.at[t, e - 1], R.s4r.at[t, e - 1], {"rep": self.rep(e)})

    def step5(self, t):
        R = self.R
        for e in (1, 2, 3):
            r = self.rep(4 - e)
            self.arrive(R.zout.at[t, r], R.s4s.at[t, e - 1], R.s4r.at[t, e - 1], {"rep": r})

    def vec1(self, l):
        R = self.R
        R.v0[l] = jnp.sum(R.vacc[12 * l : 12 * l + 12], axis=1)
        self.push(R.v0.at[l], R.v1.at[l], R.s1s.at[6 + l], R.s1r.at[6 + l], self.dev(self.p, self.core))

    def vec2(self, l):
        R, t = self.R, 6 + l
        self.arrive(R.v1.at[l], R.s1s.at[t], R.s1r.at[t], self.dev(self.p, self.core))
        R.v2[l] = R.v0[l] + R.v1[l]
        for k in (1, 2, 3):
            self.push(R.v2.at[l], R.v3.at[l, k - 1], R.s2s.at[t, k - 1], R.s2r.at[t, k - 1], self.dev(self.chip[k], self.c))

    def vec3(self, l):
        R, t = self.R, 6 + l
        tot = R.v2[l]
        for k in (1, 2, 3):
            self.arrive(R.v3.at[l, k - 1], R.s2s.at[t, k - 1], R.s2r.at[t, k - 1], self.dev(self.chip[k], self.c))
            tot = tot + R.v3[l, k - 1]
        R.v4[l, self.z] = tot
        for e in (1, 2, 3):
            here = R.v4.at[l, self.z]
            self.push(here, here, R.s3s.at[t, e - 1], R.s3r.at[t, e - 1], {"rep": self.rep(e)})

    def vec4(self, l):
        R, t = self.R, 6 + l
        for e in (1, 2, 3):
            r = self.rep(4 - e)
            self.arrive(R.v4.at[l, r], R.s3s.at[t, e - 1], R.s3r.at[t, e - 1], {"rep": r})
        R.vout[12 * l : 12 * l + 12, :] = (R.v4[l, 0] + R.v4[l, 1]) + (R.v4[l, 2] + R.v4[l, 3])

    def place_vectors(self):
        R = self.R
        R.pk[...] = jnp.zeros(R.pk.shape, F32)
        n = R.small[0].shape[1]
        for l in range(2):
            for k, ref in enumerate(R.small[:8]):
                R.pk[12 * l + k : 12 * l + k + 1, :n] = ref[l : l + 1, :].astype(F32)
        row = lax.broadcasted_iota(jnp.int32, (128, 384), 0)
        col = lax.broadcasted_iota(jnp.int32, (128, 384), 1)
        put = (col == row + n * self.f) & (row < n)
        R.mine[...] = nn(R.pk[...].astype(BF16), put.astype(F32).astype(BF16))
        ub = R.small[8]
        w = ub.shape[1]
        row = lax.broadcasted_iota(jnp.int32, (w, 384), 0)
        col = lax.broadcasted_iota(jnp.int32, (w, 384), 1)
        put = (col == row + w * lax.rem(self.f, 2)).astype(F32).astype(BF16)
        moved = nn(ub[...], put)
        for l in range(2):
            for h in range(4):
                R.mine[12 * l + 8 + h : 12 * l + 9 + h, :] = moved[l : l + 1, :] * (self.p == h).astype(F32)


def single_kernel(names, *refs):
    R = NS(**dict(zip(names, refs)))
    R.rows = R.x.shape[0]
    R.datt, R.g = R.att, R.gin
    R.grad = lambda k, l: (R.dD, R.dU, R.dA)[k].at[l]
    compute(R, (R.x, R.mid, R.out), lambda *a: None)
    R.vg[...] = jnp.sum(R.vacc[...], axis=1)


def single(x, cot, seg, vec, wqkv, wo, wup, wd):
    (rows, d), f = x.shape, wd.shape[1]
    sc = scratch_single(rows, d, f)
    names = ("x", "cot", "seg", "vec", "wqkv", "wo", "wup", "wd", "out", "gin", "dA", "dU", "dD", "vg", *sc)
    s = jax.ShapeDtypeStruct
    return pl.pallas_call(
        functools.partial(single_kernel, names),
        out_shape=(
            s((rows, d), F32), s((rows, d), F32), s((2, 2, 4, d // 8, f), BF16), s((2, 2, 4, d // 8, f), BF16),
            s((2, 2, 4, f // 8, d), BF16), s((24, d), F32)),
        in_specs=[pl.BlockSpec(memory_space=pltpu.VMEM)] * 8,
        out_specs=[pl.BlockSpec(memory_space=pltpu.VMEM)] * 6,
        scratch_shapes=list(sc.values()),
        compiler_params=pltpu.CompilerParams(vmem_limit_bytes=67043328),
    )(x, cot, seg, vec, wqkv, wo, wup, wd)


def fused_kernel(names, *refs):
    R = NS(**dict(zip(names, refs)))
    R.small = [getattr(R, "p%d" % i) for i in range(9)]
    R.rows = R.xb.shape[0]
    R.datt, R.g = R.att, R.mid
    R.grad = lambda k, l: (R.dD, R.dU, R.dA)[k]
    load = pltpu.make_async_copy(R.x, R.xb, R.io.at[0])
    load.start()
    C = Comm(R)
    C.place_vectors()
    C.barrier()
    for i in range(9):
        C.gather_start(i)
    load.wait()

    def hook(name, l):
        t = 3 * l
        if name == "qkv":
            if l == 0:
                C.gather_forward(0)
            C.gather_forward(1 + 4 * l)
            if l == 0:
                C.gather_finish(0)
                R.vec[...] = jnp.sum(R.gat[...], axis=0)
            C.gather_finish(1 + 4 * l)
        if name == "att":
            C.gather_forward(2 + 4 * l)
        if name == "mlp":
            C.gather_forward(3 + 4 * l)
            C.gather_forward(4 + 4 * l)
            for k in (2, 3, 4):
                C.gather_finish(k + 4 * l)
        if name == "fwd":
            pltpu.make_async_copy(R.xb, R.out, R.io.at[1]).start()
        if name == "b0" and l == 0:
            C.step3(5)
            C.vec2(1)
        if name == "dD":
            C.step1(t)
            if l == 0:
                C.step4(5)
                C.vec3(1)
        if name == "dU":
            C.step2(t)
            C.step1(t + 1)
        if name == "batt":
            C.step2(t + 1)
            C.step3(t)
        if name == "dA":
            C.step1(t + 2)
            C.step3(t + 1)
            C.step4(t)
        if name == "b1":
            C.vec1(l)
            C.step2(t + 2)
            C.step4(t + 1)

    compute(R, (R.xb, R.mid, R.xb), hook)
    save = pltpu.make_async_copy(R.g, R.gin, R.io.at[2])
    save.start()
    C.vec2(0)
    C.step3(2)
    C.vec3(0)
    C.step4(2)
    C.vec4(1)
    C.vec4(0)
    for t in (3, 4, 5, 0, 1, 2):
        C.step5(t)
    for cp in C.open:
        cp.wait_send()
    pltpu.make_async_copy(R.xb, R.out, R.io.at[1]).wait()
    save.wait()


def fused(x, cot, seg, small, sqkv, so, sup, sd):
    (rows, d), f = x.shape, 8 * sd.shape[1]
    sc = dict(xb=pltpu.VMEM((rows, d), F32), io=pltpu.SemaphoreType.DMA((3,)), **scratch_single(rows, d, f), **scratch_comm(d, f))
    ins = ("x", "cot", "seg", *("p%d" % i for i in range(9)), "sqkv", "so", "sup", "sd")
    names = (*ins, "out", "gin", "zout", "vout", *sc)
    s = jax.ShapeDtypeStruct
    any_, vm = pl.BlockSpec(memory_space=pl.ANY), pl.BlockSpec(memory_space=pltpu.VMEM)
    return pl.pallas_call(
        functools.partial(fused_kernel, names),
        out_shape=(s((rows, d), F32), s((rows, d), F32), s((6, 4, d // 8, d), BF16), s((24, d), F32)),
        in_specs=[any_] + [vm] * 11 + [any_] * 4,
        out_specs=[any_, any_, vm, vm],
        scratch_shapes=list(sc.values()),
        compiler_params=pltpu.CompilerParams(vmem_limit_bytes=67043328, collective_id=0, has_side_effects=True),
    )(x, cot, seg, *small, sqkv, so, sup, sd)


def finish_kernel(*refs):
    out, gin, zout, vout = refs[:4]
    o_out, o_gin, n1g, n1b, qkv, qb, vb, wo, ob, n2g, n2b, up, ub, down, db, buf, sem = refs[4:]
    loads = [pltpu.make_async_copy(src, buf.at[i], sem.at[i]) for i, src in enumerate((out, gin))]
    saves = [pltpu.make_async_copy(buf.at[i], dst, sem.at[i + 2]) for i, dst in enumerate((o_out, o_gin))]
    for cp in loads:
        cp.start()
    f = lax.axis_index("fsdp")
    s, w = zout.shape[2:]
    for l in range(2):
        for j in range(4):
            if j < 3:
                qkv[l, :, w * j : w * j + w] = zout[3 * l + 2, j].astype(F32)
            else:
                wo[l] = zout[3 * l + 2, j].astype(F32)
            up[l, :, w * j : w * j + w] = zout[3 * l + 1, j].astype(F32)
            down[l, s * j : s * j + s, :] = zout[3 * l, j].astype(F32)
    v = pltpu.roll(vout[...], lax.rem(w - s * f, w), 1)
    u = vout[8:12, :]
    half = 4 * s * lax.rem(f, 2)
    for l in range(2):
        for k, ref in enumerate((n1g, n1b, qb, vb, ob, n2g, n2b, db)):
            ref[l : l + 1, :] = v[12 * l + k : 12 * l + k + 1, :s]
        row = vout[pl.ds(12 * l + 8 + f // 2, 1), :]
        ub[l : l + 1, :] = pltpu.roll(jnp.broadcast_to(row, (8, w)), lax.rem(w - half, w), 1)[:1, : 4 * s]
    for a, b in zip(loads, saves):
        a.wait()
        b.start()
    for b in saves:
        b.wait()


def finish(out, gin, zout, vout):
    rows, d = out.shape
    s = d // 8
    t = jax.ShapeDtypeStruct
    vec = t((2, s), F32)
    any_, vm = pl.BlockSpec(memory_space=pl.ANY), pl.BlockSpec(memory_space=pltpu.VMEM)
    return pl.pallas_call(
        finish_kernel,
        out_shape=(
            t((rows, d), F32), t((rows, d), F32), vec, vec, t((2, s, 3 * d), F32), vec, vec, t((2, s, d), F32), vec, vec, vec,
            t((2, s, 4 * d), F32), t((2, 4 * s), F32), t((2, 4 * s, d), F32), vec),
        in_specs=[any_, any_, vm, vm],
        out_specs=[any_, any_] + [vm] * 13,
        scratch_shapes=[pltpu.VMEM((2, rows, d), F32), pltpu.SemaphoreType.DMA((4,))],
    )(out, gin, zout, vout)


def local_fused(x, cot, seg, n1g, n1b, qkv, qb, vb, wo, ob, n2g, n2b, up, ub, down, db):
    small = (n1g, n1b, qb, vb, ob, n2g, n2b, db, ub)
    return finish(*fused(x, cot, seg[None], small, qkv, wo, up, down))


def local_plain(x, cot, seg, n1g, n1b, qkv, qb, vb, wo, ob, n2g, n2b, up, ub, down, db):
    def gather(a):
        return lax.all_gather(a, "fsdp", axis=1, tiled=True)

    def scatter(a):
        return lax.psum(lax.psum_scatter(a, "fsdp", scatter_dimension=1, tiled=True), "rep")

    d = x.shape[1]
    vecs = jnp.stack([gather(a) for a in (n1g, n1b, qb, vb, ob, n2g, n2b, db)], 1)
    vec = jnp.concatenate([vecs, gather(ub).reshape(2, 4, d)], 1).astype(F32).reshape(24, d)
    out, gin, da, du, dd, vg = single(x, cot, seg[None], vec, gather(qkv), gather(wo), gather(up), gather(down))
    da, du, dd = (jnp.swapaxes(a, 1, 2).reshape(2, -1, a.shape[-1]).astype(F32) for a in (da, du, dd))
    da, du, dd = scatter(da), scatter(du), scatter(dd)
    vg = vg.reshape(2, 12, d)
    g = [scatter(vg[:, k]) for k in range(8)]
    gub = scatter(vg[:, 8:].reshape(2, 4 * d))
    return (out, gin, g[0], g[1], da[..., : 3 * d], g[2], g[3], da[..., 3 * d :], g[4], g[5], g[6], du, gub, dd, g[7])


def solution(mesh):
    from jax.sharding import PartitionSpec as P

    vec, mat, row = P(None, "fsdp"), P(None, "fsdp", None), P(("rep", "fsdp"), None)
    params = (vec, vec, mat, vec, vec, mat, vec, vec, vec, mat, vec, mat, vec)
    local = local_fused if dict(mesh.shape) == {"rep": 4, "fsdp": 8} else local_plain
    return jax.shard_map(local, mesh=mesh, in_specs=(row, row, P(("rep", "fsdp")), *params), out_specs=(row, row, *params), check_vma=False)
```

```python
import functools
from types import SimpleNamespace as NS
import jax
import jax.numpy as jnp
from jax import lax
from jax.experimental import pallas as pl
from jax.experimental.pallas import tpu as pltpu

HEADS = 6
HEAD_DIM = 64
IMG = 197
TILE = 256
norm_eps = 1e-06
neg_fill = -1e30
root_half = 0.7071067811865476
inv_root_tau = 0.3989422804014327
F32, BF16 = jnp.float32, jnp.bfloat16
LOG2E = 1.4426950408889634
FORE = ((0, 256), (0, 448), (192, 448), (192, 1024), (384, 1024), (384, 1024), (384, 1024), (384, 1024))
BACK = ((0, 208), (0, 400), (192, 400), (192, 592), (384, 800), (576, 800), (576, 992), (784, 992))
BASE = tuple(sum(e - s for s, e in FORE[:b]) for b in range(9))
FORE_ORDER = (4, 5, 3, 6, 7, 1, 2, 0)
BACK_ORDER = (3, 4, 6, 1, 5, 0, 2, 7)
SLOTS, SLOT = 3, 832


def nn(a, b):
    return lax.dot_general(a, b, (((1,), (0,)), ((), ())), preferred_element_type=F32)


def nt(a, b):
    return lax.dot_general(a, b, (((1,), (1,)), ((), ())), preferred_element_type=F32)


def tn(a, b):
    return lax.dot_general(a, b, (((0,), (0,)), ((), ())), preferred_element_type=F32)


def fold8(x):
    return jnp.sum(x.reshape(x.shape[0] // 8, 8, x.shape[1]), axis=0)


def norm(x):
    c = x - jnp.mean(x, -1, keepdims=True)
    r = lax.rsqrt(jnp.mean(c * c, -1, keepdims=True) + norm_eps)
    return c * r, r


def norm_back(grad, n, r, gain):
    e = grad * gain
    return r * (e - jnp.mean(e, -1, keepdims=True) - n * jnp.mean(e * n, -1, keepdims=True))


def gelu_both(pre):
    cdf = 0.5 * lax.erf(pre * root_half) + 0.5
    return pre * cdf, cdf + (pre * inv_root_tau) * jnp.exp2(pre * pre * (-0.5 * LOG2E))


def vrow(R, l, k):
    return R.vec[12 * l + k : 12 * l + k + 1, :]


def add_sum(R, l, k, x):
    R.vacc[12 * l + k] += fold8(x)


def stage_qkv(R, l, src):
    gain, bias, qb, vb = (vrow(R, l, k) for k in range(4))

    def tile(i, c):
        rows = pl.ds(pl.multiple_of(i * TILE, TILE), TILE)
        n, r = norm(src[rows, :])
        R.n1[l, rows, :] = n.astype(BF16)
        R.stats[l, rows, 0:1] = r
        a = (n * gain + bias).astype(BF16)
        R.aT[l, :, rows] = a.T
        proj = nn(a, R.wqkv[l])
        R.q[l, rows, :] = ((proj[:, :384] + qb) * (HEAD_DIM**-0.5 * LOG2E)).astype(BF16)
        R.k[l, rows, :] = proj[:, 384:768].astype(BF16)
        R.v[l, rows, :] = (proj[:, 768:] + vb).astype(BF16)
        return c

    lax.fori_loop(0, R.rows // TILE, tile, 0)


def stack_heads(x, low):
    zero = jnp.zeros_like(x)
    return jnp.concatenate([jnp.where(low, x, zero), jnp.where(low, zero, x)], 0)


def lowlanes():
    return lax.broadcasted_iota(jnp.int32, (1, 128), 1) < HEAD_DIM

def twice(x):
    return jnp.concatenate([x, x], 1)

def stage_attend(R, l):
    low = lowlanes()

    def pair(pr, c):
        lanes = pl.ds(pl.multiple_of(pr * 128, 128), 128)

        def scores(i, b):
            s, e = FORE[b]
            q = stack_heads(R.q[l, 128 * b : 128 * b + 128, lanes], low)
            R.fb[i % SLOTS, : e - s, :] = nt(R.k[l, s:e, lanes], q)

        def finish(i, b):
            s, e = FORE[b]
            x = R.fb[i % SLOTS, : e - s, :] + twice(R.bias[BASE[b] : BASE[b + 1], :])
            top = jnp.max(x, 0, keepdims=True)
            p = jnp.exp2(x - top)
            den = jnp.sum(p, 0, keepdims=True)
            p = p.astype(BF16)
            vt = R.v[l, s:e, lanes].T
            inv = 1.0 / den
            o = jnp.concatenate([nn(vt[:64], p[:, :128]) * inv[:, :128], nn(vt[64:], p[:, 128:]) * inv[:, 128:]], 0)
            R.att[128 * b : 128 * b + 128, lanes] = o.T.astype(BF16)
            e = top + jnp.log2(den)
            R.lse[l, pr, 0:1, 128 * b : 128 * b + 128] = e[:, :128]
            R.lse[l, pr, 1:2, 128 * b : 128 * b + 128] = e[:, 128:]

        order = FORE_ORDER
        for i, b in enumerate(order):
            scores(i, b)
            if i >= SLOTS - 1:
                finish(i - SLOTS + 1, order[i - SLOTS + 1])
        for i in range(len(order) - SLOTS + 1, len(order)):
            finish(i, order[i])
        return c

    lax.fori_loop(0, 3, pair, 0)

def stage_mlp(R, l, src, dst):
    ob, gain, bias, db = (vrow(R, l, k) for k in (4, 5, 6, 7))
    ub = jnp.concatenate([vrow(R, l, 8 + ch) for ch in range(4)], 1)
    last = R.rows // TILE - 1

    def project(rows):
        att = R.att[rows, :]
        R.attT[l, :, rows] = att.T
        return src[rows, :] + nn(att, R.wo[l]) + ob

    def prepare(rows, mid):
        n, r = norm(mid)
        R.n2[l, rows, :] = n.astype(BF16)
        R.stats[l, rows, 1:2] = r
        m = (n * gain + bias).astype(BF16)
        R.mT[l, :, rows] = m.T
        R.gml[:TILE, :] = m
        R.midb[...] = mid + db

    def tile(i, c):
        rows = pl.ds(pl.multiple_of(i * TILE, TILE), TILE)
        after = pl.ds(pl.multiple_of(jnp.minimum(i + 1, last) * TILE, TILE), TILE)
        base = R.midb[...]
        hid, slope = gelu_both(nn(R.gml[:TILE, :], R.wup[l]) + ub)
        hid = hid.astype(BF16)
        R.slope[l, rows, :] = slope.astype(BF16)
        prepare(after, project(after))
        dst[rows, :] = base + nn(hid, R.wd[l])
        R.hidT[l, :, rows] = hid.T
        return c

    start = pl.ds(0, TILE)
    prepare(start, project(start))
    lax.fori_loop(0, last + 1, tile, 0)


def stage_mlp_back(R, l):
    gain = vrow(R, l, 5)

    def tile(i, c):
        rows = pl.ds(pl.multiple_of(i * TILE, TILE), TILE)
        g = R.g[rows, :]
        gl = R.gl[rows, :]
        add_sum(R, l, 7, g)
        dm = jnp.zeros_like(g)
        for ch in range(4):
            cols = slice(384 * ch, 384 * ch + 384)
            dpre = nt(gl, R.wd[l, cols, :]) * R.slope[l, rows, cols].astype(F32)
            add_sum(R, l, 8 + ch, dpre)
            dpre = dpre.astype(BF16)
            R.slope[l, rows, cols] = dpre
            dm = dm + nt(dpre, R.wup[l, :, cols])
        n = R.n2[l, rows, :].astype(F32)
        add_sum(R, l, 5, dm * n)
        add_sum(R, l, 6, dm)
        gm = g + norm_back(dm, n, R.stats[l, rows, 1:2], gain)
        add_sum(R, l, 4, gm)
        R.g[rows, :] = gm
        gml = gm.astype(BF16)
        R.gml[rows, :] = gml
        R.datt[rows, :] = nt(gml, R.wo[l]).astype(BF16)
        return c

    lax.fori_loop(0, R.rows // TILE, tile, 0)


def stage_weight_down(R, l):
    def block(b, c):
        rows = pl.ds(pl.multiple_of(b * n, n), n)
        R.grad(0, l)[lax.rem(b, 2), b // 2] = nn(R.hidT[l, rows, :], R.gl[...]).astype(BF16)
        return c

    n = R.hidT.shape[1] // 8
    lax.fori_loop(0, 8, block, 0)


def put_rows(ref, cols, x):
    n = x.shape[0] // 8
    for b in range(8):
        ref[b % 2, b // 2, :, cols] = x[n * b : n * b + n].astype(BF16)


def stage_weight_up(R, l):
    def block(b, c):
        cols = pl.ds(pl.multiple_of(b * 256, 256), 256)
        put_rows(R.grad(1, l), cols, nn(R.mT[l], R.slope[l, :, cols]))
        return c

    lax.fori_loop(0, 6, block, 0)


def stage_weight_out(R, l):
    put_rows(R.grad(2, l), slice(1152, 1536), nn(R.attT[l], R.gml[...]))


def stage_weight_qkv(R, l):
    def block(b, c):
        cols = pl.ds(pl.multiple_of(b * 384, 128), 384)
        put_rows(R.grad(2, l), cols, nn(R.aT[l], R.dproj[:, cols]))
        return c

    lax.fori_loop(0, 3, block, 0)


def stage_attend_back(R, l):
    low = lowlanes()

    def pair(pr, c):
        off = pl.multiple_of(pr * 128, 128)
        lanes = pl.ds(off, 128)
        R.dk[...] = jnp.zeros((R.rows, 128), F32)
        R.dv[...] = jnp.zeros((R.rows, 128), F32)

        def scores(i, b):
            s, e = BACK[b]
            rows = slice(128 * b, 128 * b + 128)
            R.fb[i % SLOTS, : e - s, :] = nt(R.k[l, s:e, lanes], stack_heads(R.q[l, rows, lanes], low))
            R.fb[i % SLOTS, 416 : 416 + e - s, :] = nt(R.v[l, s:e, lanes], stack_heads(R.datt[rows, lanes], low))

        def finish(i, b):
            s, e = BACK[b]
            rows = slice(128 * b, 128 * b + 128)
            base = BASE[b] + s - FORE[b][0]
            lse = jnp.concatenate([R.lse[l, pr, 0:1, rows], R.lse[l, pr, 1:2, rows]], 1)
            x = R.fb[i % SLOTS, : e - s, :] + twice(R.bias[base : base + e - s, :])
            p = jnp.exp2(x - lse)
            dp = R.fb[i % SLOTS, 416 : 416 + e - s, :]
            delta = jnp.sum(p * dp, 0, keepdims=True)
            ds = (p * (dp - delta)).astype(BF16)
            p = p.astype(BF16)
            R.dv[s:e, :] += nn(p, stack_heads(R.datt[rows, lanes], low))
            R.dk[s:e, :] += nn(ds, stack_heads(R.q[l, rows, lanes], low))
            kt = R.k[l, s:e, lanes].T
            dq = jnp.concatenate([nn(kt[:64], ds[:, :128]), nn(kt[64:], ds[:, 128:])], 0).T * (HEAD_DIM**-0.5)
            R.vacc[12 * l + 2, :, lanes] += fold8(dq)
            R.dproj[rows, lanes] = dq.astype(BF16)

        order = BACK_ORDER
        for i, b in enumerate(order):
            scores(i, b)
            if i >= SLOTS - 1:
                finish(i - SLOTS + 1, order[i - SLOTS + 1])
        for i in range(len(order) - SLOTS + 1, len(order)):
            finish(i, order[i])
        dv = R.dv[...]
        R.vacc[12 * l + 3, :, lanes] += fold8(dv)
        R.dproj[:, pl.ds(384 + off, 128)] = (R.dk[...] * (1.0 / LOG2E)).astype(BF16)
        R.dproj[:, pl.ds(768 + off, 128)] = dv.astype(BF16)
        return c

    lax.fori_loop(0, 3, pair, 0)

def stage_qkv_back(R, l):
    gain = vrow(R, l, 0)

    def tile(i, c):
        rows = pl.ds(pl.multiple_of(i * TILE, TILE), TILE)
        da = nt(R.dproj[rows, :], R.wqkv[l])
        n = R.n1[l, rows, :].astype(F32)
        add_sum(R, l, 0, da * n)
        add_sum(R, l, 1, da)
        g = R.g[rows, :] + norm_back(da, n, R.stats[l, rows, 0:1], gain)
        R.g[rows, :] = g
        if l:
            R.gl[rows, :] = g.astype(BF16)
        return c

    lax.fori_loop(0, R.rows // TILE, tile, 0)


def stage_segments(R):
    seg = R.seg[...].astype(F32)
    cols = jnp.broadcast_to(seg, (128, R.rows)).T
    R.stats[0, :, 2:3] = cols[:, :1]
    for b in range(8):
        i, j = FORE[b]
        R.bias[BASE[b] : BASE[b + 1], :] = jnp.where(cols[i:j] == seg[:, 128 * b : 128 * b + 128], 0.0, neg_fill)


def stage_cotangent(R):
    def tile(i, c):
        rows = pl.ds(pl.multiple_of(i * TILE, TILE), TILE)
        g = jnp.where(R.stats[0, rows, 2:3] >= 0.0, R.cot[rows, :], 0.0)
        R.g[rows, :] = g
        R.gl[rows, :] = g.astype(BF16)
        return c

    lax.fori_loop(0, R.rows // TILE, tile, 0)


def compute(R, streams, hook):
    R.vacc[...] = jnp.zeros(R.vacc.shape, F32)
    stage_segments(R)
    for l in range(2):
        hook("qkv", l)
        stage_qkv(R, l, streams[l])
        hook("att", l)
        stage_attend(R, l)
        hook("mlp", l)
        stage_mlp(R, l, streams[l], streams[l + 1])
    hook("fwd", 0)
    stage_cotangent(R)
    for l in (1, 0):
        stage_weight_down(R, l)
        hook("dD", l)
        stage_mlp_back(R, l)
        hook("b0", l)
        stage_weight_up(R, l)
        hook("dU", l)
        stage_weight_out(R, l)
        hook("dO", l)
        stage_attend_back(R, l)
        hook("batt", l)
        stage_weight_qkv(R, l)
        hook("dA", l)
        stage_qkv_back(R, l)
        hook("b1", l)


MESH = pl.DeviceIdType.MESH
VECTORS = 8


def scratch_single(rows, d, f):
    v = pltpu.VMEM
    return dict(
        mid=v((rows, d), F32), n1=v((2, rows, d), BF16), n2=v((2, rows, d), BF16),
        stats=v((2, rows, 128), F32), aT=v((2, d, rows), BF16),
        q=v((2, rows, d), BF16), k=v((2, rows, d), BF16), v=v((2, rows, d), BF16),
        att=v((rows, d), BF16), attT=v((2, d, rows), BF16), mT=v((2, d, rows), BF16),
        hidT=v((2, f, rows), BF16), slope=v((2, rows, f), BF16),
        bias=v((BASE[8], 128), F32), lse=v((2, 3, 2, rows), F32), fb=v((SLOTS, SLOT, 256), F32),
        midb=v((TILE, d), F32),
        gl=v((rows, d), BF16), gml=v((rows, d), BF16),
        dproj=v((rows, 3 * d), BF16), vacc=v((24, 8, d), F32),
    )


def scratch_comm(d, f):
    v, dma = pltpu.VMEM, pltpu.SemaphoreType.DMA
    s, t = d // 8, f // 8
    return dict(
        wqkv=v((2, d, 3 * d), BF16), wo=v((2, d, d), BF16), wup=v((2, d, f), BF16), wd=v((2, f, d), BF16),
        pk=v((24, 128), F32), mine=v((24, d), F32), gat=v((8, 24, d), F32), vec=v((24, d), F32),
        dD=v((2, 4, t, d), BF16), dU=v((2, 4, s, f), BF16), dA=v((2, 4, s, f), BF16),
        pD=v((2, 4, t, d), BF16), pU=v((2, 4, s, f), BF16), pA=v((2, 4, s, f), BF16),
        xD=v((2, 3, t, d), BF16), xU=v((2, 3, s, f), BF16), xA=v((2, 3, s, f), BF16),
        zb=v((6, 4, s, d), BF16), zr=v((6, 4, s, d), BF16), zs=v((6, s, d), BF16),
        v0=v((2, 12, d), F32), v1=v((2, 12, d), F32), v2=v((2, 12, d), F32), v3=v((2, 3, 12, d), F32), v4=v((2, 4, 12, d), F32), vs=v((2, 12, d), F32), vl=dma((2,)),
        loc=dma((9,)), ags=dma((9, 7)), agr=dma((9, 7)), s1s=dma((8,)), s1r=dma((8,)), s2s=dma((8, 3)), s2r=dma((8, 3)),
        s3s=dma((8, 3)), s3r=dma((8, 3)), s4s=dma((6, 3)), s4r=dma((6, 3)), s4l=dma((6,)),
    )


class Comm:
    def __init__(self, R):
        self.R = R
        self.f = lax.axis_index("fsdp")
        self.z = lax.axis_index("rep")
        f = self.f
        self.c = lax.rem(f, 2)
        self.p = f // 2
        dx = 1 - 2 * lax.rem(self.p, 2)
        dy = 2 - 4 * (self.p // 2)
        self.chip = (self.p, self.p + dx, self.p + dy, self.p + dx + dy)
        self.core = 1 - self.c
        self.open, self.first = [], {}

    def dev(self, chip, core):
        return {"fsdp": 2 * chip + core}

    def rep(self, d):
        return lax.rem(self.z + d, 4)

    def push(self, src, dst, ss, rs, dev, keep=True):
        cp = pltpu.make_async_remote_copy(src, dst, ss, rs, device_id=dev, device_id_type=MESH)
        cp.start()
        if keep:
            self.open.append(cp)
        return cp

    def arrive(self, dst, ss, rs, dev):
        pltpu.make_async_remote_copy(dst, dst, ss, rs, device_id=dev, device_id_type=MESH).wait_recv()

    def barrier(self):
        bar = pltpu.get_barrier_semaphore()
        for dev in self.peers():
            pl.semaphore_signal(bar, inc=1, device_id=dev, device_id_type=MESH)
        pl.semaphore_wait(bar, 7)

    def peers(self):
        out = [self.dev(self.p, self.core)]
        out += [self.dev(self.chip[k], self.c) for k in (1, 2, 3)]
        out += [{"rep": self.rep(d)} for d in (1, 2, 3)]
        return out

    def slot(self, i, f):
        R = self.R
        if i == 0:
            return R.gat.at[f]
        l, k = (i - 1) // 4, (i - 1) % 4
        ref = (R.wqkv, R.wo, R.wup, R.wd)[k]
        n = ref.shape[1] // 8
        return ref.at[l, pl.ds(pl.multiple_of(f * n, n), n)]

    def source(self, i):
        R = self.R
        if i == 0:
            return R.mine
        l, k = (i - 1) // 4, (i - 1) % 4
        return (R.sqkv, R.so, R.sup, R.sd)[k].at[l]

    def gather_start(self, i):
        R, src, dst = self.R, self.source(i), self.slot(i, self.f)
        self.push(src, dst, R.ags.at[i, 1], R.agr.at[i, 1], self.dev(self.chip[1], self.c))
        self.push(src, dst, R.ags.at[i, 2], R.agr.at[i, 2], self.dev(self.chip[2], self.c))
        self.push(src, dst, R.ags.at[i, 3], R.agr.at[i, 3], self.dev(self.chip[3], self.c))
        self.push(src, dst, R.ags.at[i, 0], R.agr.at[i, 0], self.dev(self.p, self.core))
        pltpu.make_async_copy(src, dst, R.loc.at[i]).start()

    def gather_forward(self, i):
        R = self.R
        for k in (1, 2, 3):
            own = self.slot(i, 2 * self.chip[k] + self.c)
            self.arrive(own, R.ags.at[i, k], R.agr.at[i, k], self.dev(self.chip[k], self.c))
            self.push(own, own, R.ags.at[i, 3 + k], R.agr.at[i, 3 + k], self.dev(self.p, self.core))

    def gather_finish(self, i):
        R = self.R
        pltpu.make_async_copy(self.source(i), self.slot(i, self.f), R.loc.at[i]).wait()
        for k in (0, 1, 2, 3):
            j = 0 if k == 0 else 3 + k
            dst = self.slot(i, 2 * self.chip[k] + self.core)
            self.arrive(dst, R.ags.at[i, j], R.agr.at[i, j], self.dev(self.p, self.core))

    def grads(self, t):
        R, l = self.R, t // 3
        d, p, x = ((R.dD, R.pD, R.xD), (R.dU, R.pU, R.xU), (R.dA, R.pA, R.xA))[t % 3]
        return d, p.at[l], x.at[l]

    def step1(self, t):
        R = self.R
        d, p, x = self.grads(t)
        self.first[t] = self.push(d.at[self.core], p, R.s1s.at[t], R.s1r.at[t], self.dev(self.p, self.core), False)

    def step2(self, t):
        R = self.R
        d, p, x = self.grads(t)
        self.first[t].wait()
        for k in (3, 1, 2, 0):
            ch = self.chip[k]
            p[ch] = (d[self.c, ch].astype(F32) + p[ch].astype(F32)).astype(BF16)
            if k:
                self.push(p.at[ch], x.at[k - 1], R.s2s.at[t, k - 1], R.s2r.at[t, k - 1], self.dev(ch, self.c))

    def step3(self, t):
        R = self.R
        d, p, x = self.grads(t)
        for k in (1, 2, 3):
            self.arrive(x.at[k - 1], R.s2s.at[t, k - 1], R.s2r.at[t, k - 1], self.dev(self.chip[k], self.c))
        s = R.zb.shape[2]
        w = R.zb.shape[3]
        for j in range(4):
            at = (slice(s * j, s * j + s), slice(None)) if t % 3 == 0 else (slice(None), slice(w * j, w * j + w))
            tot = p[(self.p, *at)].astype(F32)
            for k in range(3):
                tot = tot + x[(k, *at)].astype(F32)
            R.zb[t, j] = tot.astype(BF16)
        for e in (1, 2, 3):
            r = self.rep(e)
            self.push(R.zb.at[t, r], R.zr.at[t, self.z], R.s3s.at[t, e - 1], R.s3r.at[t, e - 1], {"rep": r})

    def step4(self, t):
        R = self.R
        tot = R.zb[t, self.z].astype(F32)
        for e in (1, 2, 3):
            r = self.rep(4 - e)
            self.arrive(R.zr.at[t, r], R.s3s.at[t, e - 1], R.s3r.at[t, e - 1], {"rep": r})
            tot = tot + R.zr[t, r].astype(F32)
        R.zs[t] = tot.astype(BF16)
        here = R.zout.at[t, self.z]
        for e in (1, 2, 3):
            self.push(R.zs.at[t], here, R.s4s.at[t, e - 1], R.s4r.at[t, e - 1], {"rep": self.rep(e)})
        pltpu.make_async_copy(R.zs.at[t], here, R.s4l.at[t]).start()

    def step5(self, t):
        R = self.R
        for e in (1, 2, 3):
            r = self.rep(4 - e)
            self.arrive(R.zout.at[t, r], R.s4s.at[t, e - 1], R.s4r.at[t, e - 1], {"rep": r})
        pltpu.make_async_copy(R.zs.at[t], R.zout.at[t, self.z], R.s4l.at[t]).wait()

    def late_sends(self):
        for cp in self.open:
            cp.wait_send()

    def late_io(self, save):
        pltpu.make_async_copy(self.R.xb, self.R.out, self.R.io.at[1]).wait()
        save.wait()
        for l in range(2):
            pltpu.make_async_copy(self.R.vs.at[l], self.R.vout.at[l], self.R.vl.at[l]).wait()

    def vec1(self, l):
        R = self.R
        R.v0[l] = jnp.sum(R.vacc[12 * l : 12 * l + 12], axis=1)
        self.push(R.v0.at[l], R.v1.at[l], R.s1s.at[6 + l], R.s1r.at[6 + l], self.dev(self.p, self.core))

    def vec2(self, l):
        R, t = self.R, 6 + l
        self.arrive(R.v1.at[l], R.s1s.at[t], R.s1r.at[t], self.dev(self.p, self.core))
        R.v2[l] = R.v0[l] + R.v1[l]
        for k in (1, 2, 3):
            self.push(R.v2.at[l], R.v3.at[l, k - 1], R.s2s.at[t, k - 1], R.s2r.at[t, k - 1], self.dev(self.chip[k], self.c))

    def vec3(self, l):
        R, t = self.R, 6 + l
        tot = R.v2[l]
        for k in (1, 2, 3):
            self.arrive(R.v3.at[l, k - 1], R.s2s.at[t, k - 1], R.s2r.at[t, k - 1], self.dev(self.chip[k], self.c))
            tot = tot + R.v3[l, k - 1]
        R.v4[l, self.z] = tot
        for e in (1, 2, 3):
            here = R.v4.at[l, self.z]
            self.push(here, here, R.s3s.at[t, e - 1], R.s3r.at[t, e - 1], {"rep": self.rep(e)})

    def vec4(self, l):
        R, t = self.R, 6 + l
        for e in (1, 2, 3):
            r = self.rep(4 - e)
            self.arrive(R.v4.at[l, r], R.s3s.at[t, e - 1], R.s3r.at[t, e - 1], {"rep": r})
        R.vs[l] = (R.v4[l, 0] + R.v4[l, 1]) + (R.v4[l, 2] + R.v4[l, 3])
        pltpu.make_async_copy(R.vs.at[l], R.vout.at[l], R.vl.at[l]).start()

    def place_vectors(self):
        R = self.R
        R.pk[...] = jnp.zeros(R.pk.shape, F32)
        n = R.small[0].shape[1]
        for l in range(2):
            for k, ref in enumerate(R.small[:8]):
                R.pk[12 * l + k : 12 * l + k + 1, :n] = ref[l : l + 1, :].astype(F32)
        row = lax.broadcasted_iota(jnp.int32, (128, 384), 0)
        col = lax.broadcasted_iota(jnp.int32, (128, 384), 1)
        put = (col == row + n * self.f) & (row < n)
        R.mine[...] = nn(R.pk[...].astype(BF16), put.astype(F32).astype(BF16))
        ub = R.small[8]
        w = ub.shape[1]
        row = lax.broadcasted_iota(jnp.int32, (w, 384), 0)
        col = lax.broadcasted_iota(jnp.int32, (w, 384), 1)
        put = (col == row + w * lax.rem(self.f, 2)).astype(F32).astype(BF16)
        moved = nn(ub[...], put)
        for l in range(2):
            for h in range(4):
                R.mine[12 * l + 8 + h : 12 * l + 9 + h, :] = moved[l : l + 1, :] * (self.p == h).astype(F32)


def single_kernel(names, *refs):
    R = NS(**dict(zip(names, refs)))
    R.rows = R.x.shape[0]
    R.datt, R.g = R.att, R.gin
    R.dk, R.dv = R.dkv.at[0], R.dkv.at[1]
    R.grad = lambda k, l: (R.dD, R.dU, R.dA)[k].at[l]
    compute(R, (R.x, R.mid, R.out), lambda *a: None)
    R.vg[...] = jnp.sum(R.vacc[...], axis=1)


def single(x, cot, seg, vec, wqkv, wo, wup, wd):
    (rows, d), f = x.shape, wd.shape[1]
    sc = dict(dkv=pltpu.VMEM((2, rows, 128), F32), **scratch_single(rows, d, f))
    names = ("x", "cot", "seg", "vec", "wqkv", "wo", "wup", "wd", "out", "gin", "dA", "dU", "dD", "vg", *sc)
    s = jax.ShapeDtypeStruct
    return pl.pallas_call(
        functools.partial(single_kernel, names),
        out_shape=(
            s((rows, d), F32), s((rows, d), F32), s((2, 2, 4, d // 8, f), BF16), s((2, 2, 4, d // 8, f), BF16),
            s((2, 2, 4, f // 8, d), BF16), s((24, d), F32)),
        in_specs=[pl.BlockSpec(memory_space=pltpu.VMEM)] * 8,
        out_specs=[pl.BlockSpec(memory_space=pltpu.VMEM)] * 6,
        scratch_shapes=list(sc.values()),
        compiler_params=pltpu.CompilerParams(vmem_limit_bytes=67043328),
    )(x, cot, seg, vec, wqkv, wo, wup, wd)


PLAN = {
    ("dD", 1): (("step1", 3),),
    ("b0", 1): (("step2", 3),),
    ("dU", 1): (("step1", 4),),
    ("batt", 1): (("step2", 4), ("step3", 3)),
    ("dA", 1): (("step1", 5),),
    ("b1", 1): (("vec1", 1), ("step2", 5), ("step4", 3)),
    ("dD", 0): (("step1", 0), ("step3", 4), ("vec2", 1)),
    ("b0", 0): (("step2", 0), ("step3", 5), ("step4", 4), ("vec3", 1)),
    ("dU", 0): (("step1", 1),),
    ("dO", 0): (("step2", 1),),
    ("batt", 0): (("step3", 0), ("step4", 5), ("vec4", 1)),
    ("dA", 0): (("step1", 2),),
    ("b1", 0): (("vec1", 0), ("step2", 2), ("step3", 1), ("step4", 0)),
    ("tail", 0): (("vec2", 0), ("step3", 2), ("vec3", 0), ("step4", 1), ("step4", 2), ("vec4", 0)),
}


def fused_kernel(names, *refs):
    R = NS(**dict(zip(names, refs)))
    R.small = [getattr(R, "p%d" % i) for i in range(9)]
    R.rows = R.xb.shape[0]
    R.datt, R.g = R.att, R.mid
    R.dk, R.dv = R.cot.at[:, :128], R.cot.at[:, 128:256]
    R.grad = lambda k, l: (R.dD, R.dU, R.dA)[k]
    load = pltpu.make_async_copy(R.x, R.xb, R.io.at[0])
    load.start()
    cot = pltpu.make_async_copy(R.hcot, R.cot, R.io.at[3])
    cot.start()
    C = Comm(R)
    C.place_vectors()
    C.barrier()
    for i in range(9):
        C.gather_start(i)
    load.wait()

    def hook(name, l):
        t = 3 * l
        if name == "qkv":
            if l == 0:
                C.gather_forward(0)
            C.gather_forward(1 + 4 * l)
            if l == 0:
                C.gather_finish(0)
                R.vec[...] = jnp.sum(R.gat[...], axis=0)
            C.gather_finish(1 + 4 * l)
        if name == "att":
            C.gather_forward(2 + 4 * l)
        if name == "mlp":
            C.gather_forward(3 + 4 * l)
            C.gather_forward(4 + 4 * l)
            for k in (2, 3, 4):
                C.gather_finish(k + 4 * l)
        if name == "fwd":
            pltpu.make_async_copy(R.xb, R.out, R.io.at[1]).start()
            cot.wait()
        for what, k in PLAN.get((name, l), ()):
            getattr(C, what)(k)

    compute(R, (R.xb, R.mid, R.xb), hook)
    save = pltpu.make_async_copy(R.g, R.gin, R.io.at[2])
    save.start()
    for what, k in PLAN["tail", 0]:
        getattr(C, what)(k)
    for t in (3, 4, 5, 0, 1, 2):
        C.step5(t)
    C.late_sends()
    C.late_io(save)


def fused(x, cot, seg, small, sqkv, so, sup, sd):
    (rows, d), f = x.shape, 8 * sd.shape[1]
    sc = dict(xb=pltpu.VMEM((rows, d), F32), cot=pltpu.VMEM((rows, d), F32), io=pltpu.SemaphoreType.DMA((4,)), **scratch_single(rows, d, f), **scratch_comm(d, f))
    ins = ("x", "hcot", "seg", *("p%d" % i for i in range(9)), "sqkv", "so", "sup", "sd")
    names = (*ins, "out", "gin", "zout", "vout", *sc)
    s = jax.ShapeDtypeStruct
    any_, vm = pl.BlockSpec(memory_space=pl.ANY), pl.BlockSpec(memory_space=pltpu.VMEM)
    return pl.pallas_call(
        functools.partial(fused_kernel, names),
        out_shape=(s((rows, d), F32), s((rows, d), F32), s((6, 4, d // 8, d), BF16), s((2, 12, d), F32)),
        in_specs=[any_] * 2 + [vm] * 10 + [any_] * 4,
        out_specs=[any_] * 4,
        scratch_shapes=list(sc.values()),
        compiler_params=pltpu.CompilerParams(vmem_limit_bytes=67043328, collective_id=0, has_side_effects=True),
    )(x, cot, seg, *small, sqkv, so, sup, sd)


def finish_kernel(*refs):
    ins, outs = refs[:4], refs[4:19]
    zb, vb, buf, sem = refs[-4:]
    vals = refs[19:-4]
    rows = buf.shape[1]
    load = [pltpu.make_async_copy(ins[i], dst, sem.at[i]) for i, dst in ((2, zb), (3, vb), (0, buf.at[0]), (1, buf.at[1]))]
    for cp in load:
        cp.start()
    save = [pltpu.make_async_copy(src, dst, sem.at[4 + i]) for i, (src, dst) in enumerate(zip((buf.at[0], buf.at[1], *vals), outs))]
    n1g, n1b, qkv, qb, vbias, wo, ob, n2g, n2b, up, ub, down, db = vals
    f = lax.axis_index("fsdp")
    s, w = zb.shape[2:]
    load[0].wait()
    for l in range(2):
        for j in range(4):
            up[l, :, w * j : w * j + w] = zb[3 * l + 1, j].astype(F32)
    save[11].start()
    for l in range(2):
        for j in range(4):
            down[l, s * j : s * j + s, :] = zb[3 * l, j].astype(F32)
    save[13].start()
    for l in range(2):
        for j in range(3):
            qkv[l, :, w * j : w * j + w] = zb[3 * l + 2, j].astype(F32)
        wo[l] = zb[3 * l + 2, 3].astype(F32)
    save[4].start()
    save[7].start()
    for i in (0, 1):
        load[2 + i].wait()
        save[i].start()
    load[1].wait()
    shift = lax.rem(w - 4 * s * lax.rem(f, 2), w)
    for l in range(2):
        v = pltpu.roll(vb[l], lax.rem(w - s * f, w), 1)
        for k, ref in enumerate((n1g, n1b, qb, vbias, ob, n2g, n2b, db)):
            ref[l : l + 1, :] = v[k : k + 1, :s]
        row = vb[l, pl.ds(8 + f // 2, 1), :]
        ub[l : l + 1, :] = pltpu.roll(jnp.broadcast_to(row, (8, w)), shift, 1)[:1, : 4 * s]
    for i in (2, 3, 5, 6, 8, 9, 10, 12, 14):
        save[i].start()
    for cp in save:
        cp.wait()


def finish(out, gin, zout, vout):
    rows, d = out.shape
    s = d // 8
    shapes = ((2, s), (2, s), (2, s, 3 * d), (2, s), (2, s), (2, s, d), (2, s), (2, s), (2, s), (2, s, 4 * d), (2, 4 * s), (2, 4 * s, d), (2, s))
    any_ = pl.BlockSpec(memory_space=pl.ANY)
    return pl.pallas_call(
        finish_kernel,
        out_shape=[jax.ShapeDtypeStruct(t, F32) for t in ((rows, d), (rows, d), *shapes)],
        in_specs=[any_] * 4,
        out_specs=[any_] * 15,
        scratch_shapes=[pltpu.VMEM(t, F32) for t in shapes]
        + [pltpu.VMEM(zout.shape, BF16), pltpu.VMEM(vout.shape, F32), pltpu.VMEM((2, rows, d), F32), pltpu.SemaphoreType.DMA((19,))],
    )(out, gin, zout, vout)


def local_fused(x, cot, seg, n1g, n1b, qkv, qb, vb, wo, ob, n2g, n2b, up, ub, down, db):
    small = (n1g, n1b, qb, vb, ob, n2g, n2b, db, ub)
    return finish(*fused(x, cot, seg[None], small, qkv, wo, up, down))


def local_plain(x, cot, seg, n1g, n1b, qkv, qb, vb, wo, ob, n2g, n2b, up, ub, down, db):
    def gather(a):
        return lax.all_gather(a, "fsdp", axis=1, tiled=True)

    def scatter(a):
        return lax.psum(lax.psum_scatter(a, "fsdp", scatter_dimension=1, tiled=True), "rep")

    d = x.shape[1]
    vecs = jnp.stack([gather(a) for a in (n1g, n1b, qb, vb, ob, n2g, n2b, db)], 1)
    vec = jnp.concatenate([vecs, gather(ub).reshape(2, 4, d)], 1).astype(F32).reshape(24, d)
    out, gin, da, du, dd, vg = single(x, cot, seg[None], vec, gather(qkv), gather(wo), gather(up), gather(down))
    da, du, dd = (jnp.swapaxes(a, 1, 2).reshape(2, -1, a.shape[-1]).astype(F32) for a in (da, du, dd))
    da, du, dd = scatter(da), scatter(du), scatter(dd)
    vg = vg.reshape(2, 12, d)
    g = [scatter(vg[:, k]) for k in range(8)]
    gub = scatter(vg[:, 8:].reshape(2, 4 * d))
    return (out, gin, g[0], g[1], da[..., : 3 * d], g[2], g[3], da[..., 3 * d :], g[4], g[5], g[6], du, gub, dd, g[7])


def solution(mesh):
    from jax.sharding import PartitionSpec as P

    vec, mat, row = P(None, "fsdp"), P(None, "fsdp", None), P(("rep", "fsdp"), None)
    params = (vec, vec, mat, vec, vec, mat, vec, vec, vec, mat, vec, mat, vec)
    local = local_fused if dict(mesh.shape) == {"rep": 4, "fsdp": 8} else local_plain
    return jax.shard_map(local, mesh=mesh, in_specs=(row, row, P(("rep", "fsdp")), *params), out_specs=(row, row, *params), check_vma=False)
```

```python
import functools
from types import SimpleNamespace as NS
import jax
import jax.numpy as jnp
from jax import lax
from jax.experimental import pallas as pl
from jax.experimental.pallas import tpu as pltpu

HEADS = 6
HEAD_DIM = 64
IMG = 197
TILE, BIG = 256, 512
norm_eps = 1e-06
neg_fill = -1e30
root_half = 0.7071067811865476
inv_root_tau = 0.3989422804014327
F32, BF16 = jnp.float32, jnp.bfloat16
LOG2E = 1.4426950408889634
FORE = ((0, 256), (0, 448), (192, 448), (192, 1024), (384, 1024), (384, 1024), (384, 1024), (384, 1024))
BACK = ((0, 208), (0, 400), (192, 400), (192, 592), (384, 800), (576, 800), (576, 992), (784, 992))
BASE = tuple(sum(e - s for s, e in FORE[:b]) for b in range(9))
FORE_ORDER = (4, 5, 3, 6, 7, 1, 2, 0)
BACK_ORDER = (3, 4, 6, 1, 5, 0, 2, 7)
SLOTS, SLOT = 3, 832


def nn(a, b):
    return lax.dot_general(a, b, (((1,), (0,)), ((), ())), preferred_element_type=F32)


def nt(a, b):
    return lax.dot_general(a, b, (((1,), (1,)), ((), ())), preferred_element_type=F32)


def tn(a, b):
    return lax.dot_general(a, b, (((0,), (0,)), ((), ())), preferred_element_type=F32)


def fold8(x):
    return jnp.sum(x.reshape(x.shape[0] // 8, 8, x.shape[1]), axis=0)


def norm(x):
    c = x - jnp.mean(x, -1, keepdims=True)
    r = lax.rsqrt(jnp.mean(c * c, -1, keepdims=True) + norm_eps)
    return c * r, r


def norm_back(grad, n, r, gain):
    e = grad * gain
    return r * (e - jnp.mean(e, -1, keepdims=True) - n * jnp.mean(e * n, -1, keepdims=True))


def gelu_both(pre):
    cdf = 0.5 * lax.erf(pre * root_half) + 0.5
    return pre * cdf, cdf + (pre * inv_root_tau) * jnp.exp2(pre * pre * (-0.5 * LOG2E))


def vrow(R, l, k):
    return R.vec[12 * l + k : 12 * l + k + 1, :]


def add_sum(R, l, k, x):
    R.vacc[12 * l + k] += fold8(x)


def stage_qkv(R, l, src):
    gain, bias, qb, vb = (vrow(R, l, k) for k in range(4))

    def tile(i, c):
        rows = pl.ds(pl.multiple_of(i * BIG, BIG), BIG)
        n, r = norm(src[rows, :])
        R.n1[l, rows, :] = n.astype(BF16)
        R.stats[l, rows, 0:1] = r
        a = (n * gain + bias).astype(BF16)
        R.aT[l, :, rows] = a.T
        proj = nn(a, R.wqkv[l])
        R.q[l, rows, :] = ((proj[:, :384] + qb) * (HEAD_DIM**-0.5 * LOG2E)).astype(BF16)
        R.k[l, rows, :] = proj[:, 384:768].astype(BF16)
        R.v[l, rows, :] = (proj[:, 768:] + vb).astype(BF16)
        return c

    lax.fori_loop(0, R.rows // BIG, tile, 0)


def stack_heads(x, low):
    zero = jnp.zeros_like(x)
    return jnp.concatenate([jnp.where(low, x, zero), jnp.where(low, zero, x)], 0)


def lowlanes():
    return lax.broadcasted_iota(jnp.int32, (1, 128), 1) < HEAD_DIM

def twice(x):
    return jnp.concatenate([x, x], 1)

def when_is(index, hook, name, l, points):
    for k in points:
        pl.when(index == k)(functools.partial(hook, name + str(k), l))


def stage_attend(R, l, hook):
    low = lowlanes()

    def pair(pr, c):
        when_is(pr, hook, "att", l, (1, 2))
        lanes = pl.ds(pl.multiple_of(pr * 128, 128), 128)

        def scores(i, b):
            s, e = FORE[b]
            q = stack_heads(R.q[l, 128 * b : 128 * b + 128, lanes], low)
            R.fb[i % SLOTS, : e - s, :] = nt(R.k[l, s:e, lanes], q)

        def finish(i, b):
            s, e = FORE[b]
            x = R.fb[i % SLOTS, : e - s, :] + twice(R.bias[BASE[b] : BASE[b + 1], :])
            top = jnp.max(x, 0, keepdims=True)
            p = jnp.exp2(x - top)
            den = jnp.sum(p, 0, keepdims=True)
            p = p.astype(BF16)
            vt = R.v[l, s:e, lanes].T
            inv = 1.0 / den
            o = jnp.concatenate([nn(vt[:64], p[:, :128]) * inv[:, :128], nn(vt[64:], p[:, 128:]) * inv[:, 128:]], 0)
            R.att[128 * b : 128 * b + 128, lanes] = o.T.astype(BF16)
            e = top + jnp.log2(den)
            R.lse[l, pr, 0:1, 128 * b : 128 * b + 128] = e[:, :128]
            R.lse[l, pr, 1:2, 128 * b : 128 * b + 128] = e[:, 128:]

        order = FORE_ORDER
        for i, b in enumerate(order):
            scores(i, b)
            if i >= SLOTS - 1:
                finish(i - SLOTS + 1, order[i - SLOTS + 1])
        for i in range(len(order) - SLOTS + 1, len(order)):
            finish(i, order[i])
        return c

    lax.fori_loop(0, 3, pair, 0)

def stage_mlp(R, l, src, dst, hook):
    ob, gain, bias, db = (vrow(R, l, k) for k in (4, 5, 6, 7))
    ub = jnp.concatenate([vrow(R, l, 8 + ch) for ch in range(4)], 1)
    last = R.rows // TILE - 1

    def project(rows):
        att = R.att[rows, :]
        R.attT[l, :, rows] = att.T
        return src[rows, :] + nn(att, R.wo[l]) + ob

    def prepare(rows, mid):
        n, r = norm(mid)
        R.n2[l, rows, :] = n.astype(BF16)
        R.stats[l, rows, 1:2] = r
        m = (n * gain + bias).astype(BF16)
        R.mT[l, :, rows] = m.T
        R.gml[:TILE, :] = m
        R.midb[...] = mid + db

    def tile(i, c):
        when_is(i, hook, "mlp", l, (1, 2, 3))
        rows = pl.ds(pl.multiple_of(i * TILE, TILE), TILE)
        after = pl.ds(pl.multiple_of(jnp.minimum(i + 1, last) * TILE, TILE), TILE)
        base = R.midb[...]
        hid, slope = gelu_both(nn(R.gml[:TILE, :], R.wup[l]) + ub)
        hid = hid.astype(BF16)
        R.slope[l, rows, :] = slope.astype(BF16)
        prepare(after, project(after))
        dst[rows, :] = base + nn(hid, R.wd[l])
        R.hidT[l, :, rows] = hid.T
        return c

    start = pl.ds(0, TILE)
    prepare(start, project(start))
    lax.fori_loop(0, last + 1, tile, 0)


def stage_mlp_back(R, l, hook):
    gain = vrow(R, l, 5)

    def tile(i, c):
        when_is(i, hook, "b0t", l, (1, 2, 3))
        rows = pl.ds(pl.multiple_of(i * TILE, TILE), TILE)
        g = R.g[rows, :]
        gl = R.gl[rows, :]
        add_sum(R, l, 7, g)
        dpre = nt(gl, R.wd[l]) * R.slope[l, rows, :].astype(F32)
        for ch in range(4):
            add_sum(R, l, 8 + ch, dpre[:, 384 * ch : 384 * ch + 384])
        dpre = dpre.astype(BF16)
        R.slope[l, rows, :] = dpre
        dm = nt(dpre, R.wup[l])
        n = R.n2[l, rows, :].astype(F32)
        add_sum(R, l, 5, dm * n)
        add_sum(R, l, 6, dm)
        gm = g + norm_back(dm, n, R.stats[l, rows, 1:2], gain)
        add_sum(R, l, 4, gm)
        R.g[rows, :] = gm
        gml = gm.astype(BF16)
        R.gml[rows, :] = gml
        R.datt[rows, :] = nt(gml, R.wo[l]).astype(BF16)
        return c

    lax.fori_loop(0, R.rows // TILE, tile, 0)


def stage_weight_down(R, l):
    n = R.hidT.shape[1] // 8

    def block(b, c):
        x = nn(R.hidT[l, pl.ds(pl.multiple_of(b * 4 * n, 4 * n), 4 * n), :], R.gl[...]).astype(BF16)
        for k in range(4):
            R.grad(0, l)[k % 2, 2 * b + k // 2] = x[n * k : n * k + n]
        return c

    lax.fori_loop(0, 2, block, 0)


def put_rows(ref, cols, x):
    n = x.shape[0] // 8
    for b in range(8):
        ref[b % 2, b // 2, :, cols] = x[n * b : n * b + n].astype(BF16)


def stage_weight_up(R, l):
    def block(b, c):
        cols = pl.ds(pl.multiple_of(b * 512, 512), 512)
        put_rows(R.grad(1, l), cols, nn(R.mT[l], R.slope[l, :, cols]))
        return c

    lax.fori_loop(0, 3, block, 0)


def put_block(R, l, j, x):
    n = x.shape[0] // 8
    ref = R.grad(2, l)
    for b in range(8):
        ref[j, b % 2, b // 2] = x[n * b : n * b + n].astype(BF16)


def stage_weight_out(R, l):
    put_block(R, l, 3, nn(R.attT[l], R.gml[...]))


def weight_qkv(R, l, pr):
    off = pr * 128 if isinstance(pr, int) else pl.multiple_of(pr * 128, 128)
    put_block(R, l, pr, nn(R.aT[l], jnp.concatenate([R.dproj[:, pl.ds(384 * k + off, 128)] for k in range(3)], 1)))


def stage_attend_back(R, l, hook, pairs=None):
    low = lowlanes()

    def pair(pr, c):
        off = pr * 128 if isinstance(pr, int) else pl.multiple_of(pr * 128, 128)
        lanes = pl.ds(off, 128)
        if pairs is None:
            when_is(pr, hook, "pr", l, (1, 2))
        R.dk[...] = jnp.zeros((R.rows, 128), F32)
        R.dv[...] = jnp.zeros((R.rows, 128), F32)

        def scores(i, b):
            s, e = BACK[b]
            rows = slice(128 * b, 128 * b + 128)
            R.fb[i % SLOTS, : e - s, :] = nt(R.k[l, s:e, lanes], stack_heads(R.q[l, rows, lanes], low))
            R.fb[i % SLOTS, 416 : 416 + e - s, :] = nt(R.v[l, s:e, lanes], stack_heads(R.datt[rows, lanes], low))

        def finish(i, b):
            s, e = BACK[b]
            rows = slice(128 * b, 128 * b + 128)
            base = BASE[b] + s - FORE[b][0]
            lse = jnp.concatenate([R.lse[l, pr, 0:1, rows], R.lse[l, pr, 1:2, rows]], 1)
            x = R.fb[i % SLOTS, : e - s, :] + twice(R.bias[base : base + e - s, :])
            p = jnp.exp2(x - lse)
            dp = R.fb[i % SLOTS, 416 : 416 + e - s, :]
            delta = jnp.sum(p * dp, 0, keepdims=True)
            ds = (p * (dp - delta)).astype(BF16)
            p = p.astype(BF16)
            R.dv[s:e, :] += nn(p, stack_heads(R.datt[rows, lanes], low))
            R.dk[s:e, :] += nn(ds, stack_heads(R.q[l, rows, lanes], low))
            kt = R.k[l, s:e, lanes].T
            dq = jnp.concatenate([nn(kt[:64], ds[:, :128]), nn(kt[64:], ds[:, 128:])], 0).T * (HEAD_DIM**-0.5)
            R.vacc[12 * l + 2, :, lanes] += fold8(dq)
            R.dproj[rows, lanes] = dq.astype(BF16)

        order = BACK_ORDER
        for i, b in enumerate(order):
            scores(i, b)
            if i >= SLOTS - 1:
                finish(i - SLOTS + 1, order[i - SLOTS + 1])
        for i in range(len(order) - SLOTS + 1, len(order)):
            finish(i, order[i])
        dv = R.dv[...]
        R.vacc[12 * l + 3, :, lanes] += fold8(dv)
        R.dproj[:, pl.ds(384 + off, 128)] = (R.dk[...] * (1.0 / LOG2E)).astype(BF16)
        R.dproj[:, pl.ds(768 + off, 128)] = dv.astype(BF16)
        weight_qkv(R, l, pr)
        return c

    if pairs is None:
        lax.fori_loop(0, 3, pair, 0)
    else:
        pair(pairs, 0)

def stage_qkv_back(R, l, lo=0, hi=2):
    gain = vrow(R, l, 0)

    def tile(i, c):
        rows = pl.ds(pl.multiple_of(i * BIG, BIG), BIG)
        da = nt(R.dproj[rows, :], R.wqkv[l])
        n = R.n1[l, rows, :].astype(F32)
        add_sum(R, l, 0, da * n)
        add_sum(R, l, 1, da)
        g = R.g[rows, :] + norm_back(da, n, R.stats[l, rows, 0:1], gain)
        R.g[rows, :] = g
        if l:
            R.gl[rows, :] = g.astype(BF16)
        return c

    lax.fori_loop(lo, hi, tile, 0)


def stage_segments(R):
    seg = R.seg[...].astype(F32)
    cols = jnp.broadcast_to(seg, (128, R.rows)).T
    R.stats[0, :, 2:3] = cols[:, :1]
    for b in range(8):
        i, j = FORE[b]
        R.bias[BASE[b] : BASE[b + 1], :] = jnp.where(cols[i:j] == seg[:, 128 * b : 128 * b + 128], 0.0, neg_fill)


def stage_cotangent(R):
    def tile(i, c):
        rows = pl.ds(pl.multiple_of(i * TILE, TILE), TILE)
        g = jnp.where(R.stats[0, rows, 2:3] >= 0.0, R.cot[rows, :], 0.0)
        R.g[rows, :] = g
        R.gl[rows, :] = g.astype(BF16)
        return c

    lax.fori_loop(0, R.rows // TILE, tile, 0)


def compute(R, streams, hook):
    R.vacc[...] = jnp.zeros(R.vacc.shape, F32)
    stage_segments(R)
    for l in range(2):
        hook("qkv", l)
        stage_qkv(R, l, streams[l])
        hook("att", l)
        stage_attend(R, l, hook)
        hook("mlp", l)
        stage_mlp(R, l, streams[l], streams[l + 1], hook)
    hook("fwd", 0)
    stage_cotangent(R)
    for l in (1, 0):
        stage_weight_down(R, l)
        hook("dD", l)
        stage_mlp_back(R, l, hook)
        hook("b0", l)
        stage_weight_up(R, l)
        hook("dU", l)
        stage_weight_out(R, l)
        hook("dO", l)
        if l:
            stage_attend_back(R, l, hook)
            hook("pair2", l)
        else:
            for pr in range(3):
                stage_attend_back(R, l, hook, pr)
                hook("pair" + str(pr), l)
        stage_qkv_back(R, l, 0, 1)
        hook("half", l)
        stage_qkv_back(R, l, 1, 2)
        hook("b1", l)


MESH = pl.DeviceIdType.MESH
VECTORS = 8


def scratch_single(rows, d, f):
    v = pltpu.VMEM
    return dict(
        mid=v((rows, d), F32), n1=v((2, rows, d), BF16), n2=v((2, rows, d), BF16),
        stats=v((2, rows, 128), F32), aT=v((2, d, rows), BF16),
        q=v((2, rows, d), BF16), k=v((2, rows, d), BF16), v=v((2, rows, d), BF16),
        att=v((rows, d), BF16), attT=v((2, d, rows), BF16), mT=v((2, d, rows), BF16),
        hidT=v((2, f, rows), BF16), slope=v((2, rows, f), BF16),
        bias=v((BASE[8], 128), F32), lse=v((2, 3, 2, rows), F32), fb=v((SLOTS, SLOT, 256), F32),
        midb=v((TILE, d), F32),
        gl=v((rows, d), BF16), gml=v((rows, d), BF16),
        dproj=v((rows, 3 * d), BF16), vacc=v((24, 8, d), F32),
    )


def scratch_comm(d, f):
    v, dma = pltpu.VMEM, pltpu.SemaphoreType.DMA
    s, t = d // 8, f // 8
    return dict(
        wqkv=v((2, d, 3 * d), BF16), wo=v((2, d, d), BF16), wup=v((2, d, f), BF16), wd=v((2, f, d), BF16),
        pk=v((24, 128), F32), mine=v((24, d), BF16), gat=v((8, 24, d), BF16), vec=v((24, d), F32),
        dD=v((2, 4, t, d), BF16), dU=v((2, 4, s, f), BF16), dA=v((4, 2, 4, s, d), BF16),
        pD=v((2, 4, t, d), BF16), pU=v((2, 4, s, f), BF16), pA=v((8, 4, s, d), BF16),
        xD=v((2, 3, t, d), BF16), xU=v((2, 3, s, f), BF16), xA=v((8, 3, s, d), BF16),
        zb=v((4, 4, s, d), BF16), zr=v((4, 3, s, d), BF16), zs=v((4, s, d), BF16),
        yb=v((8, s, d), BF16), yr=v((8, 3, s, d), BF16), ys=v((8, s, d), BF16),
        v0=v((2, 12, d), F32), v1=v((2, 12, d), F32), v2=v((2, 12, d), F32), v3=v((2, 3, 12, d), F32), v4=v((2, 4, 12, d), F32),
        vs=v((2, 12, d), F32), vl=dma((2,)), loc=dma((9,)), ags=dma((9,)), agr=dma((9, 3)),
        s1s=dma((14,)), s1r=dma((14,)), s2s=dma((14,)), s2r=dma((14,)), s3s=dma((14,)), s3r=dma((14,)), s4s=dma((12,)), s4r=dma((12,)),
    )


OWNER = (0, 3, 1, 2)


class Comm:
    def __init__(self, R):
        self.R = R
        self.f = lax.axis_index("fsdp")
        self.z = lax.axis_index("rep")
        f = self.f
        self.c = lax.rem(f, 2)
        self.p = f // 2
        dx = 1 - 2 * lax.rem(self.p, 2)
        dy = 2 - 4 * (self.p // 2)
        self.chip = (self.p, self.p + dx, self.p + dy, self.p + dx + dy)
        self.core = 1 - self.c
        self.partner = self.dev(self.p, self.core)
        self.steps = (
            self.own, self.relay, self.diagonal, self.have, self.step1, self.step2, self.step3, self.step4, self.step5,
            self.vec1, self.vec2, self.vec3, self.vec4)

    def dev(self, chip, core):
        return {"fsdp": 2 * chip + core}

    def rep(self, d):
        return lax.rem(self.z + d, 4)

    def push(self, src, dst, ss, rs, dev):
        pltpu.make_async_remote_copy(src, dst, ss, rs, device_id=dev, device_id_type=MESH).start()

    def got(self, ref, sem):
        pltpu.make_async_remote_copy(ref, ref, sem, sem, device_id=self.partner, device_id_type=MESH).wait_recv()

    def sent(self, ref, sem):
        pltpu.make_async_remote_copy(ref, ref, sem, sem, device_id=self.partner, device_id_type=MESH).wait_send()

    def barrier(self):
        bar = pltpu.get_barrier_semaphore()
        for dev in self.peers():
            pl.semaphore_signal(bar, inc=1, device_id=dev, device_id_type=MESH)
        pl.semaphore_wait(bar, 7)

    def peers(self):
        out = [self.partner]
        out += [self.dev(self.chip[k], self.c) for k in (1, 2, 3)]
        out += [{"rep": self.rep(d)} for d in (1, 2, 3)]
        return out

    def shards(self, i, f, n=1):
        R = self.R
        if i == 0:
            return R.gat.at[pl.ds(f, n)]
        l, k = (i - 1) // 4, (i - 1) % 4
        ref = (R.wqkv, R.wo, R.wup, R.wd)[k]
        m = ref.shape[1] // 8
        return ref.at[l, pl.ds(pl.multiple_of(f * m, m), n * m)]

    def half(self, i, f, h):
        R = self.R
        l, k = (i - 1) // 4, (i - 1) % 4
        ref = (R.wqkv, R.wo, R.wup, R.wd)[k]
        m, w = ref.shape[1] // 8, ref.shape[2]
        cut = w // 256 * 128
        return ref.at[l, pl.ds(pl.multiple_of(f * m, m), m), pl.ds(0, cut) if h == 0 else pl.ds(cut, w - cut)]

    def source(self, i):
        R = self.R
        if i == 0:
            return R.mine
        l, k = (i - 1) // 4, (i - 1) % 4
        return (R.sqkv, R.so, R.sup, R.sd)[k].at[l]

    def target(self, i):
        return self.R.gat.at[self.f] if i == 0 else self.shards(i, self.f)

    def own(self, i):
        R, src, dst = self.R, self.source(i), self.target(i)
        for k in (1, 2, 3) if i < 2 else (1, 2):
            self.push(src, dst, R.ags.at[i], R.agr.at[i, 0], self.dev(self.chip[k], self.c))
        self.push(src, dst, R.ags.at[i], R.agr.at[i, 2], self.partner)
        pltpu.make_async_copy(src, dst, R.loc.at[i]).start()

    def forward(self, i, k):
        here = self.shards(i, 2 * self.chip[k] + self.c)
        self.push(here, here, self.R.ags.at[i], self.R.agr.at[i, 2], self.partner)

    def relay(self, i):
        R = self.R
        self.got(self.shards(i, 0, 3 if i < 2 else 2), R.agr.at[i, 0])
        if i >= 2:
            for h, (src, to) in enumerate(((1, 2), (2, 1))):
                here = self.half(i, 2 * self.chip[src] + self.c, h)
                self.push(here, here, R.ags.at[i], R.agr.at[i, 1], self.dev(self.chip[to], self.c))
        for k in (1, 2, 3) if i < 2 else (1, 2):
            self.forward(i, k)

    def diagonal(self, i):
        self.got(self.shards(i, 0), self.R.agr.at[i, 1])
        self.forward(i, 3)

    def have(self, i):
        R = self.R
        pltpu.make_async_copy(self.source(i), self.target(i), R.loc.at[i]).wait()
        self.got(self.shards(i, 0, 4), R.agr.at[i, 2])

    def grads(self, t):
        R = self.R
        if t < 4:
            l = t // 2
            d, p, x = ((R.dD, R.pD, R.xD), (R.dU, R.pU, R.xU))[t % 2]
            return d, p.at[l], x.at[l]
        return R.dA.at[t % 4], R.pA.at[t - 4], R.xA.at[t - 4]

    def step1(self, t):
        R = self.R
        d, p, x = self.grads(t)
        self.push(d.at[self.core], p, R.s1s.at[t], R.s1r.at[t], self.partner)

    def step2(self, t):
        R = self.R
        d, p, x = self.grads(t)
        self.sent(d.at[self.core], R.s1s.at[t])
        self.got(p, R.s1r.at[t])
        for k in (3, 1, 2, 0):
            ch = self.chip[k]
            p[ch] = (d[self.c, ch].astype(F32) + p[ch].astype(F32)).astype(BF16)
            if k:
                self.push(p.at[ch], x.at[k - 1], R.s2s.at[t], R.s2r.at[t], self.dev(ch, self.c))

    def step3(self, t):
        R = self.R
        d, p, x = self.grads(t)
        self.got(x, R.s2r.at[t])
        self.sent(x, R.s2s.at[t])

        def total(*at):
            tot = p[(self.p, *at)].astype(F32)
            for k in range(3):
                tot = tot + x[(k, *at)].astype(F32)
            return tot.astype(BF16)

        s, w = R.zb.shape[2:]
        if t >= 4:
            u, owner = t - 4, OWNER[t % 4]
            R.yb[u] = total(slice(None), slice(None))

            @pl.when(self.z != owner)
            def _():
                slot = lax.rem(self.z + 3 - owner, 4)
                self.push(R.yb.at[u], R.yr.at[u, slot], R.s3s.at[t], R.s3r.at[t], {"rep": owner})

            return
        for j in range(4):
            rows, cols = slice(s * j, s * j + s), slice(w * j, w * j + w)
            R.zb[t, j] = total(rows, slice(None)) if t % 2 == 0 else total(slice(None), cols)
        for e in (1, 2, 3):
            r = self.rep(e)
            self.push(R.zb.at[t, r], R.zr.at[t, e - 1], R.s3s.at[t], R.s3r.at[t], {"rep": r})

    def place(self, t):
        return (t % 2 + 3 * (t // 2), None) if t < 4 else (3 * ((t - 4) // 4) + 2, t % 4)

    def step4(self, t):
        R = self.R
        row, j = self.place(t)
        if t >= 4:
            u, owner = t - 4, OWNER[t % 4]

            @pl.when(self.z == owner)
            def _():
                self.got(R.yr.at[u], R.s3r.at[t])
                tot = R.yb[u].astype(F32)
                for k in range(3):
                    tot = tot + R.yr[u, k].astype(F32)
                R.ys[u] = tot.astype(BF16)
                here = R.zout.at[row, j]
                for e in (1, 2, 3):
                    self.push(R.ys.at[u], here, R.s4s.at[t], R.s4r.at[t], {"rep": (owner + e) % 4})
                pltpu.make_async_copy(R.ys.at[u], here, R.s4r.at[t]).start()

            return
        self.got(R.zr.at[t], R.s3r.at[t])
        self.sent(R.zr.at[t], R.s3s.at[t])
        tot = R.zb[t, self.z].astype(F32)
        for k in range(3):
            tot = tot + R.zr[t, k].astype(F32)
        R.zs[t] = tot.astype(BF16)
        here = R.zout.at[row, self.z]
        for e in (1, 2, 3):
            self.push(R.zs.at[t], here, R.s4s.at[t], R.s4r.at[t], {"rep": self.rep(e)})
        pltpu.make_async_copy(R.zs.at[t], here, R.s4r.at[t]).start()

    def step5(self, t):
        R = self.R
        row, j = self.place(t)
        if t >= 4:
            u, owner = t - 4, OWNER[t % 4]
            self.got(R.zout.at[row, j], R.s4r.at[t])

            @pl.when(self.z == owner)
            def _():
                self.sent(R.yr.at[u], R.s4s.at[t])

            @pl.when(self.z != owner)
            def _():
                self.sent(R.yb.at[u], R.s3s.at[t])

            return
        self.got(R.zout.at[row], R.s4r.at[t])
        self.sent(R.zr.at[t], R.s4s.at[t])

    def vec1(self, l):
        R, t = self.R, 12 + l
        R.v0[l] = jnp.sum(R.vacc[12 * l : 12 * l + 12], axis=1)
        self.push(R.v0.at[l], R.v1.at[l], R.s1s.at[t], R.s1r.at[t], self.partner)

    def vec2(self, l):
        R, t = self.R, 12 + l
        self.got(R.v1.at[l], R.s1r.at[t])
        self.sent(R.v0.at[l], R.s1s.at[t])
        R.v2[l] = R.v0[l] + R.v1[l]
        for k in (1, 2, 3):
            self.push(R.v2.at[l], R.v3.at[l, k - 1], R.s2s.at[t], R.s2r.at[t], self.dev(self.chip[k], self.c))

    def vec3(self, l):
        R, t = self.R, 12 + l
        self.got(R.v3.at[l], R.s2r.at[t])
        self.sent(R.v3.at[l], R.s2s.at[t])
        tot = R.v2[l]
        for k in (1, 2, 3):
            tot = tot + R.v3[l, k - 1]
        R.v4[l, self.z] = tot
        here = R.v4.at[l, self.z]
        for e in (1, 2, 3):
            self.push(here, here, R.s3s.at[t], R.s3r.at[t], {"rep": self.rep(e)})

    def vec4(self, l):
        R, t = self.R, 12 + l
        self.got(R.v3.at[l], R.s3r.at[t])
        self.sent(R.v3.at[l], R.s3s.at[t])
        R.vs[l] = (R.v4[l, 0] + R.v4[l, 1]) + (R.v4[l, 2] + R.v4[l, 3])
        pltpu.make_async_copy(R.vs.at[l], R.vout.at[l], R.vl.at[l]).start()

    def late_sends(self):
        for i in range(9):
            self.sent(self.shards(i, 0, 7), self.R.ags.at[i])

    def late_io(self, save):
        R = self.R
        pltpu.make_async_copy(R.xb, R.out, R.io.at[1]).wait()
        save.wait()
        for l in range(2):
            pltpu.make_async_copy(R.vs.at[l], R.vout.at[l], R.vl.at[l]).wait()

    def place_vectors(self):
        R = self.R
        R.pk[...] = jnp.zeros(R.pk.shape, F32)
        n = R.small[0].shape[1]
        for l in range(2):
            for k, ref in enumerate(R.small[:8]):
                R.pk[12 * l + k : 12 * l + k + 1, :n] = ref[l : l + 1, :].astype(F32)
        row = lax.broadcasted_iota(jnp.int32, (128, 384), 0)
        col = lax.broadcasted_iota(jnp.int32, (128, 384), 1)
        put = (col == row + n * self.f) & (row < n)
        R.mine[...] = nn(R.pk[...].astype(BF16), put.astype(F32).astype(BF16)).astype(BF16)
        ub = R.small[8]
        w = ub.shape[1]
        row = lax.broadcasted_iota(jnp.int32, (w, 384), 0)
        col = lax.broadcasted_iota(jnp.int32, (w, 384), 1)
        put = (col == row + w * lax.rem(self.f, 2)).astype(F32).astype(BF16)
        moved = nn(ub[...], put)
        for l in range(2):
            for h in range(4):
                R.mine[12 * l + 8 + h : 12 * l + 9 + h, :] = (moved[l : l + 1, :] * (self.p == h).astype(F32)).astype(BF16)


def single_kernel(names, *refs):
    R = NS(**dict(zip(names, refs)))
    R.rows = R.x.shape[0]
    R.datt, R.g = R.att, R.gin
    R.dk, R.dv = R.dkv.at[0], R.dkv.at[1]
    R.grad = lambda k, l: (R.dD, R.dU, R.dA)[k].at[l]
    compute(R, (R.x, R.mid, R.out), lambda *a: None)
    R.vg[...] = jnp.sum(R.vacc[...], axis=1)


def single(x, cot, seg, vec, wqkv, wo, wup, wd):
    (rows, d), f = x.shape, wd.shape[1]
    sc = dict(dkv=pltpu.VMEM((2, rows, 128), F32), **scratch_single(rows, d, f))
    names = ("x", "cot", "seg", "vec", "wqkv", "wo", "wup", "wd", "out", "gin", "dA", "dU", "dD", "vg", *sc)
    s = jax.ShapeDtypeStruct
    return pl.pallas_call(
        functools.partial(single_kernel, names),
        out_shape=(
            s((rows, d), F32), s((rows, d), F32), s((2, 4, 2, 4, d // 8, d), BF16), s((2, 2, 4, d // 8, f), BF16),
            s((2, 2, 4, f // 8, d), BF16), s((24, d), F32)),
        in_specs=[pl.BlockSpec(memory_space=pltpu.VMEM)] * 8,
        out_specs=[pl.BlockSpec(memory_space=pltpu.VMEM)] * 6,
        scratch_shapes=list(sc.values()),
        compiler_params=pltpu.CompilerParams(vmem_limit_bytes=67043328),
    )(x, cot, seg, vec, wqkv, wo, wup, wd)


OWN, RELAY, DIAG, HAVE, S1, S2, S3, S4, S5, V1, V2, V3, V4 = range(13)
PLAN = {
    ("start", 0): ((OWN, 0), (OWN, 1), (OWN, 2), (OWN, 3), (OWN, 4),),
    ("qkv", 0): ((RELAY, 0), (RELAY, 1), (HAVE, 0), (HAVE, 1),),
    ("att", 0): ((RELAY, 2), (RELAY, 3),),
    ("att1", 0): ((RELAY, 4), (OWN, 5),),
    ("att2", 0): ((DIAG, 2), (DIAG, 3), (OWN, 6),),
    ("mlp", 0): ((DIAG, 4), (HAVE, 2), (HAVE, 3), (HAVE, 4),),
    ("mlp1", 0): ((RELAY, 5), (OWN, 7),),
    ("mlp2", 0): ((RELAY, 6),),
    ("mlp3", 0): ((DIAG, 5), (OWN, 8),),
    ("qkv", 1): ((HAVE, 5),),
    ("att", 1): ((RELAY, 7), (DIAG, 6),),
    ("att1", 1): ((RELAY, 8),),
    ("att2", 1): ((DIAG, 7),),
    ("mlp", 1): ((DIAG, 8), (HAVE, 6), (HAVE, 7), (HAVE, 8),),
    ("dD", 1): ((S1, 2),),
    ("b0t1", 1): ((S2, 2),),
    ("dU", 1): ((S1, 3),),
    ("dO", 1): ((S1, 11),),
    ("pr1", 1): ((S3, 2), (S2, 3), (S2, 11), (S1, 8),),
    ("pr2", 1): ((S2, 8), (S1, 9),),
    ("pair2", 1): ((S4, 2), (S2, 9), (S1, 10),),
    ("half", 1): ((S2, 10),),
    ("b1", 1): ((V1, 1),),
    ("dD", 0): ((S1, 0), (V2, 1), (S3, 3),),
    ("b0t1", 0): ((S3, 11),),
    ("b0t2", 0): ((S2, 0), (S3, 8),),
    ("b0t3", 0): ((S4, 3), (S3, 9),),
    ("b0", 0): ((S3, 10), (V3, 1), (S4, 11),),
    ("dU", 0): ((S1, 1), (S4, 8),),
    ("dO", 0): ((S1, 7), (S4, 9), (S2, 1), (S3, 0),),
    ("pair0", 0): ((S2, 7), (S1, 4), (S4, 10), (V4, 1),),
    ("pair1", 0): ((S2, 4), (S1, 5),),
    ("pair2", 0): ((S3, 1), (S2, 5), (S1, 6), (S4, 0),),
    ("half", 0): ((S3, 7), (S2, 6),),
    ("b1", 0): ((V1, 0), (S3, 4),),
    ("tail", 0): ((V2, 0), (S3, 5), (S3, 6), (V3, 0), (S4, 1), (S4, 7), (S4, 4), (S4, 5), (S4, 6), (V4, 0), (S5, 2), (S5, 3), (S5, 8), (S5, 9), (S5, 10), (S5, 11), (S5, 0), (S5, 7), (S5, 1), (S5, 4), (S5, 5), (S5, 6),),
}


def fused_kernel(names, *refs):
    R = NS(**dict(zip(names, refs)))
    R.small = [getattr(R, "p%d" % i) for i in range(9)]
    R.rows = R.xb.shape[0]
    R.datt, R.g = R.att, R.mid
    R.dk, R.dv = R.cot.at[:, :128], R.cot.at[:, 128:256]
    R.grad = lambda k, l: (R.dD, R.dU, R.dA)[k]
    load = pltpu.make_async_copy(R.x, R.xb, R.io.at[0])
    load.start()
    cot = pltpu.make_async_copy(R.hcot, R.cot, R.io.at[3])
    cot.start()
    C = Comm(R)
    C.place_vectors()
    C.barrier()

    def hook(name, l):
        for item in PLAN.get((name, l), ()):
            C.steps[item[0]](item[1])
        if (name, l) == ("qkv", 0):
            R.vec[...] = jnp.sum(R.gat[...].astype(F32), axis=0)
        if name == "fwd":
            pltpu.make_async_copy(R.xb, R.out, R.io.at[1]).start()
            cot.wait()

    hook("start", 0)
    load.wait()
    compute(R, (R.xb, R.mid, R.xb), hook)
    save = pltpu.make_async_copy(R.g, R.gin, R.io.at[2])
    save.start()
    hook("tail", 0)
    C.late_sends()
    C.late_io(save)


def fused(x, cot, seg, small, sqkv, so, sup, sd):
    (rows, d), f = x.shape, 8 * sd.shape[1]
    sc = dict(xb=pltpu.VMEM((rows, d), F32), cot=pltpu.VMEM((rows, d), F32), io=pltpu.SemaphoreType.DMA((4,)), **scratch_single(rows, d, f), **scratch_comm(d, f))
    ins = ("x", "hcot", "seg", *("p%d" % i for i in range(9)), "sqkv", "so", "sup", "sd")
    names = (*ins, "out", "gin", "zout", "vout", *sc)
    s = jax.ShapeDtypeStruct
    any_, vm = pl.BlockSpec(memory_space=pl.ANY), pl.BlockSpec(memory_space=pltpu.VMEM)
    return pl.pallas_call(
        functools.partial(fused_kernel, names),
        out_shape=(s((rows, d), F32), s((rows, d), F32), s((6, 4, d // 8, d), BF16), s((2, 12, d), F32)),
        in_specs=[any_] * 2 + [vm] * 10 + [any_] * 4,
        out_specs=[any_] * 4,
        scratch_shapes=list(sc.values()),
        compiler_params=pltpu.CompilerParams(vmem_limit_bytes=67043328, collective_id=0, has_side_effects=True),
    )(x, cot, seg, *small, sqkv, so, sup, sd)


def finish_kernel(*refs):
    ins, outs = refs[:4], refs[4:19]
    zb, vb, buf, sem = refs[-4:]
    vals = refs[19:-4]
    rows = buf.shape[1]
    load = [pltpu.make_async_copy(ins[i], dst, sem.at[i]) for i, dst in ((2, zb), (3, vb), (0, buf.at[0]), (1, buf.at[1]))]
    for cp in load:
        cp.start()
    save = [pltpu.make_async_copy(src, dst, sem.at[4 + i]) for i, (src, dst) in enumerate(zip((buf.at[0], buf.at[1], *vals), outs))]
    n1g, n1b, qkv, qb, vbias, wo, ob, n2g, n2b, up, ub, down, db = vals
    f = lax.axis_index("fsdp")
    s, w = zb.shape[2:]
    load[0].wait()
    for l in range(2):
        for j in range(4):
            up[l, :, w * j : w * j + w] = zb[3 * l + 1, j].astype(F32)
    save[11].start()
    for l in range(2):
        for j in range(4):
            down[l, s * j : s * j + s, :] = zb[3 * l, j].astype(F32)
    save[13].start()
    for l in range(2):
        for j in range(3):
            for k in range(3):
                qkv[l, :, w * k + 128 * j : w * k + 128 * j + 128] = zb[3 * l + 2, j, :, 128 * k : 128 * k + 128].astype(F32)
        wo[l] = zb[3 * l + 2, 3].astype(F32)
    save[4].start()
    save[7].start()
    for i in (0, 1):
        load[2 + i].wait()
        save[i].start()
    load[1].wait()
    shift = lax.rem(w - 4 * s * lax.rem(f, 2), w)
    for l in range(2):
        v = pltpu.roll(vb[l], lax.rem(w - s * f, w), 1)
        for k, ref in enumerate((n1g, n1b, qb, vbias, ob, n2g, n2b, db)):
            ref[l : l + 1, :] = v[k : k + 1, :s]
        row = vb[l, pl.ds(8 + f // 2, 1), :]
        ub[l : l + 1, :] = pltpu.roll(jnp.broadcast_to(row, (8, w)), shift, 1)[:1, : 4 * s]
    for i in (2, 3, 5, 6, 8, 9, 10, 12, 14):
        save[i].start()
    for cp in save:
        cp.wait()


def finish(out, gin, zout, vout):
    rows, d = out.shape
    s = d // 8
    shapes = ((2, s), (2, s), (2, s, 3 * d), (2, s), (2, s), (2, s, d), (2, s), (2, s), (2, s), (2, s, 4 * d), (2, 4 * s), (2, 4 * s, d), (2, s))
    any_ = pl.BlockSpec(memory_space=pl.ANY)
    return pl.pallas_call(
        finish_kernel,
        out_shape=[jax.ShapeDtypeStruct(t, F32) for t in ((rows, d), (rows, d), *shapes)],
        in_specs=[any_] * 4,
        out_specs=[any_] * 15,
        scratch_shapes=[pltpu.VMEM(t, F32) for t in shapes]
        + [pltpu.VMEM(zout.shape, BF16), pltpu.VMEM(vout.shape, F32), pltpu.VMEM((2, rows, d), F32), pltpu.SemaphoreType.DMA((19,))],
    )(out, gin, zout, vout)


def local_fused(x, cot, seg, n1g, n1b, qkv, qb, vb, wo, ob, n2g, n2b, up, ub, down, db):
    small = (n1g, n1b, qb, vb, ob, n2g, n2b, db, ub)
    return finish(*fused(x, cot, seg[None], small, qkv, wo, up, down))


def local_plain(x, cot, seg, n1g, n1b, qkv, qb, vb, wo, ob, n2g, n2b, up, ub, down, db):
    def gather(a):
        return lax.all_gather(a, "fsdp", axis=1, tiled=True)

    def scatter(a):
        return lax.psum(lax.psum_scatter(a, "fsdp", scatter_dimension=1, tiled=True), "rep")

    d = x.shape[1]
    vecs = jnp.stack([gather(a) for a in (n1g, n1b, qb, vb, ob, n2g, n2b, db)], 1)
    vec = jnp.concatenate([vecs, gather(ub).reshape(2, 4, d)], 1).astype(F32).reshape(24, d)
    out, gin, da, du, dd, vg = single(x, cot, seg[None], vec, gather(qkv), gather(wo), gather(up), gather(down))
    du, dd = (jnp.swapaxes(a, 1, 2).reshape(2, -1, a.shape[-1]).astype(F32) for a in (du, dd))
    da = jnp.transpose(da, (0, 3, 2, 4, 1, 5)).reshape(2, d, 4, d).astype(F32)
    dqkv = jnp.swapaxes(da[:, :, :3].reshape(2, d, 3, 3, d // 3), 2, 3).reshape(2, d, 3 * d)
    dqkv, dwo, du, dd = scatter(dqkv), scatter(da[:, :, 3]), scatter(du), scatter(dd)
    vg = vg.reshape(2, 12, d)
    g = [scatter(vg[:, k]) for k in range(8)]
    gub = scatter(vg[:, 8:].reshape(2, 4 * d))
    return (out, gin, g[0], g[1], dqkv, g[2], g[3], dwo, g[4], g[5], g[6], du, gub, dd, g[7])


def solution(mesh):
    from jax.sharding import PartitionSpec as P

    vec, mat, row = P(None, "fsdp"), P(None, "fsdp", None), P(("rep", "fsdp"), None)
    params = (vec, vec, mat, vec, vec, mat, vec, vec, vec, mat, vec, mat, vec)
    local = local_fused if dict(mesh.shape) == {"rep": 4, "fsdp": 8} else local_plain
    return jax.shard_map(local, mesh=mesh, in_specs=(row, row, P(("rep", "fsdp")), *params), out_specs=(row, row, *params), check_vma=False)
```

```python
import functools
from types import SimpleNamespace as NS
import jax
import jax.numpy as jnp
from jax import lax
from jax.experimental import pallas as pl
from jax.experimental.pallas import tpu as pltpu

HEADS = 6
HEAD_DIM = 64
IMG = 197
TILE, BIG = 256, 512
norm_eps = 1e-06
neg_fill = -1e30
root_half = 0.7071067811865476
inv_root_tau = 0.3989422804014327
F32, BF16 = jnp.float32, jnp.bfloat16
LOG2E = 1.4426950408889634
FORE = ((0, 256), (0, 448), (192, 448), (192, 1024), (384, 1024), (384, 1024), (384, 1024), (384, 1024))
BACK = ((0, 208), (0, 400), (192, 400), (192, 592), (384, 800), (576, 800), (576, 992), (784, 992))
BASE = tuple(sum(e - s for s, e in FORE[:b]) for b in range(9))
FORE_ORDER = (4, 5, 3, 6, 7, 1, 2, 0)
BACK_ORDER = (3, 4, 6, 1, 5, 0, 2, 7)
SLOTS, SLOT = 3, 832


def nn(a, b):
    return lax.dot_general(a, b, (((1,), (0,)), ((), ())), preferred_element_type=F32)


def nt(a, b):
    return lax.dot_general(a, b, (((1,), (1,)), ((), ())), preferred_element_type=F32)


def tn(a, b):
    return lax.dot_general(a, b, (((0,), (0,)), ((), ())), preferred_element_type=F32)


def fold8(x):
    return jnp.sum(x.reshape(x.shape[0] // 8, 8, x.shape[1]), axis=0)


def norm(x):
    c = x - jnp.mean(x, -1, keepdims=True)
    r = lax.rsqrt(jnp.mean(c * c, -1, keepdims=True) + norm_eps)
    return c * r, r


def norm_back(grad, n, r, gain):
    e = grad * gain
    return r * (e - jnp.mean(e, -1, keepdims=True) - n * jnp.mean(e * n, -1, keepdims=True))


def gelu_both(pre):
    cdf = 0.5 * lax.erf(pre * root_half) + 0.5
    return pre * cdf, cdf + (pre * inv_root_tau) * jnp.exp2(pre * pre * (-0.5 * LOG2E))


def vrow(R, l, k):
    return R.vec[12 * l + k : 12 * l + k + 1, :]


def add_sum(R, l, k, x):
    R.vacc[12 * l + k] += fold8(x)


def stage_qkv(R, l, src):
    gain, bias, qb, vb = (vrow(R, l, k) for k in range(4))

    def tile(i, c):
        rows = pl.ds(pl.multiple_of(i * BIG, BIG), BIG)
        n, r = norm(src[rows, :])
        R.n1[l, rows, :] = n.astype(BF16)
        R.stats[l, rows, 0:1] = r
        a = (n * gain + bias).astype(BF16)
        R.aT[l, :, rows] = a.T
        proj = nn(a, R.wqkv[l])
        R.q[l, rows, :] = ((proj[:, :384] + qb) * (HEAD_DIM**-0.5 * LOG2E)).astype(BF16)
        R.k[l, rows, :] = proj[:, 384:768].astype(BF16)
        R.v[l, rows, :] = (proj[:, 768:] + vb).astype(BF16)
        return c

    lax.fori_loop(0, R.rows // BIG, tile, 0)


def stack_heads(x, low):
    zero = jnp.zeros_like(x)
    return jnp.concatenate([jnp.where(low, x, zero), jnp.where(low, zero, x)], 0)


def lowlanes():
    return lax.broadcasted_iota(jnp.int32, (1, 128), 1) < HEAD_DIM

def twice(x):
    return jnp.concatenate([x, x], 1)

def when_is(index, hook, name, l, points):
    for k in points:
        pl.when(index == k)(functools.partial(hook, name + str(k), l))


def stage_attend(R, l, hook):
    low = lowlanes()

    def pair(pr, c):
        when_is(pr, hook, "att", l, (1, 2))
        lanes = pl.ds(pl.multiple_of(pr * 128, 128), 128)

        def scores(i, b):
            s, e = FORE[b]
            q = stack_heads(R.q[l, 128 * b : 128 * b + 128, lanes], low)
            R.fb[i % SLOTS, : e - s, :] = nt(R.k[l, s:e, lanes], q)

        def finish(i, b):
            s, e = FORE[b]
            x = R.fb[i % SLOTS, : e - s, :] + twice(R.bias[BASE[b] : BASE[b + 1], :])
            top = jnp.max(x, 0, keepdims=True)
            p = jnp.exp2(x - top)
            den = jnp.sum(p, 0, keepdims=True)
            p = p.astype(BF16)
            vt = R.v[l, s:e, lanes].T
            inv = 1.0 / den
            o = jnp.concatenate([nn(vt[:64], p[:, :128]) * inv[:, :128], nn(vt[64:], p[:, 128:]) * inv[:, 128:]], 0)
            R.att[128 * b : 128 * b + 128, lanes] = o.T.astype(BF16)
            e = top + jnp.log2(den)
            R.lse[l, pr, 0:1, 128 * b : 128 * b + 128] = e[:, :128]
            R.lse[l, pr, 1:2, 128 * b : 128 * b + 128] = e[:, 128:]

        order = FORE_ORDER
        for i, b in enumerate(order):
            scores(i, b)
            if i >= SLOTS - 1:
                finish(i - SLOTS + 1, order[i - SLOTS + 1])
        for i in range(len(order) - SLOTS + 1, len(order)):
            finish(i, order[i])
        return c

    lax.fori_loop(0, 3, pair, 0)

def stage_mlp(R, l, src, dst, hook):
    ob, gain, bias, db = (vrow(R, l, k) for k in (4, 5, 6, 7))
    ub = jnp.concatenate([vrow(R, l, 8 + ch) for ch in range(4)], 1)
    last = R.rows // TILE - 1

    def project(rows):
        att = R.att[rows, :]
        R.attT[l, :, rows] = att.T
        return src[rows, :] + nn(att, R.wo[l]) + ob

    def prepare(rows, mid):
        n, r = norm(mid)
        R.n2[l, rows, :] = n.astype(BF16)
        R.stats[l, rows, 1:2] = r
        m = (n * gain + bias).astype(BF16)
        R.mT[l, :, rows] = m.T
        R.gml[:TILE, :] = m
        R.midb[...] = mid + db

    def tile(i, c):
        when_is(i, hook, "mlp", l, (1, 2, 3))
        rows = pl.ds(pl.multiple_of(i * TILE, TILE), TILE)
        after = pl.ds(pl.multiple_of(jnp.minimum(i + 1, last) * TILE, TILE), TILE)
        base = R.midb[...]
        hid, slope = gelu_both(nn(R.gml[:TILE, :], R.wup[l]) + ub)
        hid = hid.astype(BF16)
        R.slope[l, rows, :] = slope.astype(BF16)
        prepare(after, project(after))
        dst[rows, :] = base + nn(hid, R.wd[l])
        R.hidT[l, :, rows] = hid.T
        return c

    start = pl.ds(0, TILE)
    prepare(start, project(start))
    lax.fori_loop(0, last + 1, tile, 0)


def stage_mlp_back(R, l, hook):
    gain = vrow(R, l, 5)

    def tile(i, c):
        when_is(i, hook, "b0t", l, (1, 2, 3))
        rows = pl.ds(pl.multiple_of(i * TILE, TILE), TILE)
        g = R.g[rows, :]
        gl = R.gl[rows, :]
        add_sum(R, l, 7, g)
        dpre = nt(gl, R.wd[l]) * R.slope[l, rows, :].astype(F32)
        for ch in range(4):
            add_sum(R, l, 8 + ch, dpre[:, 384 * ch : 384 * ch + 384])
        dpre = dpre.astype(BF16)
        R.slope[l, rows, :] = dpre
        dm = nt(dpre, R.wup[l])
        n = R.n2[l, rows, :].astype(F32)
        add_sum(R, l, 5, dm * n)
        add_sum(R, l, 6, dm)
        gm = g + norm_back(dm, n, R.stats[l, rows, 1:2], gain)
        add_sum(R, l, 4, gm)
        R.g[rows, :] = gm
        gml = gm.astype(BF16)
        R.gml[rows, :] = gml
        R.datt[rows, :] = nt(gml, R.wo[l]).astype(BF16)
        return c

    lax.fori_loop(0, R.rows // TILE, tile, 0)


def stage_weight_down(R, l):
    n = R.hidT.shape[1] // 8

    def block(b, c):
        x = nn(R.hidT[l, pl.ds(pl.multiple_of(b * 4 * n, 4 * n), 4 * n), :], R.gl[...]).astype(BF16)
        for k in range(4):
            R.grad(0, l)[k % 2, 2 * b + k // 2] = x[n * k : n * k + n]
        return c

    lax.fori_loop(0, 2, block, 0)


def put_rows(ref, cols, x):
    n = x.shape[0] // 8
    for b in range(8):
        ref[b % 2, b // 2, :, cols] = x[n * b : n * b + n].astype(BF16)


def stage_weight_up(R, l):
    def block(b, c):
        cols = pl.ds(pl.multiple_of(b * 512, 512), 512)
        put_rows(R.grad(1, l), cols, nn(R.mT[l], R.slope[l, :, cols]))
        return c

    lax.fori_loop(0, 3, block, 0)


def put_block(R, l, j, x):
    n = x.shape[0] // 8
    ref = R.grad(2, l)
    for b in range(8):
        ref[j, b % 2, b // 2] = x[n * b : n * b + n].astype(BF16)


def stage_weight_out(R, l):
    put_block(R, l, 3, nn(R.attT[l], R.gml[...]))


def weight_qkv(R, l, pr):
    off = pr * 128 if isinstance(pr, int) else pl.multiple_of(pr * 128, 128)
    put_block(R, l, pr, nn(R.aT[l], jnp.concatenate([R.dproj[:, pl.ds(384 * k + off, 128)] for k in range(3)], 1)))


def stage_attend_back(R, l, hook, pairs=None):
    low = lowlanes()

    def pair(pr, c):
        off = pr * 128 if isinstance(pr, int) else pl.multiple_of(pr * 128, 128)
        lanes = pl.ds(off, 128)
        if pairs is None:
            when_is(pr, hook, "pr", l, (1, 2))
        R.dk[...] = jnp.zeros((R.rows, 128), F32)
        R.dv[...] = jnp.zeros((R.rows, 128), F32)

        def scores(i, b):
            s, e = BACK[b]
            rows = slice(128 * b, 128 * b + 128)
            R.fb[i % SLOTS, : e - s, :] = nt(R.k[l, s:e, lanes], stack_heads(R.q[l, rows, lanes], low))
            R.fb[i % SLOTS, 416 : 416 + e - s, :] = nt(R.v[l, s:e, lanes], stack_heads(R.datt[rows, lanes], low))

        def finish(i, b):
            s, e = BACK[b]
            rows = slice(128 * b, 128 * b + 128)
            base = BASE[b] + s - FORE[b][0]
            lse = jnp.concatenate([R.lse[l, pr, 0:1, rows], R.lse[l, pr, 1:2, rows]], 1)
            x = R.fb[i % SLOTS, : e - s, :] + twice(R.bias[base : base + e - s, :])
            p = jnp.exp2(x - lse)
            dp = R.fb[i % SLOTS, 416 : 416 + e - s, :]
            delta = jnp.sum(p * dp, 0, keepdims=True)
            ds = (p * (dp - delta)).astype(BF16)
            p = p.astype(BF16)
            R.dv[s:e, :] += nn(p, stack_heads(R.datt[rows, lanes], low))
            R.dk[s:e, :] += nn(ds, stack_heads(R.q[l, rows, lanes], low))
            kt = R.k[l, s:e, lanes].T
            dq = jnp.concatenate([nn(kt[:64], ds[:, :128]), nn(kt[64:], ds[:, 128:])], 0).T * (HEAD_DIM**-0.5)
            R.vacc[12 * l + 2, :, lanes] += fold8(dq)
            R.dproj[rows, lanes] = dq.astype(BF16)

        order = BACK_ORDER
        for i, b in enumerate(order):
            scores(i, b)
            if i >= SLOTS - 1:
                finish(i - SLOTS + 1, order[i - SLOTS + 1])
        for i in range(len(order) - SLOTS + 1, len(order)):
            finish(i, order[i])
        dv = R.dv[...]
        R.vacc[12 * l + 3, :, lanes] += fold8(dv)
        R.dproj[:, pl.ds(384 + off, 128)] = (R.dk[...] * (1.0 / LOG2E)).astype(BF16)
        R.dproj[:, pl.ds(768 + off, 128)] = dv.astype(BF16)
        weight_qkv(R, l, pr)
        return c

    if pairs is None:
        lax.fori_loop(0, 3, pair, 0)
    else:
        pair(pairs, 0)

def stage_qkv_back(R, l, lo=0, hi=2):
    gain = vrow(R, l, 0)

    def tile(i, c):
        rows = pl.ds(pl.multiple_of(i * BIG, BIG), BIG)
        da = nt(R.dproj[rows, :], R.wqkv[l])
        n = R.n1[l, rows, :].astype(F32)
        add_sum(R, l, 0, da * n)
        add_sum(R, l, 1, da)
        g = R.g[rows, :] + norm_back(da, n, R.stats[l, rows, 0:1], gain)
        R.g[rows, :] = g
        if l:
            R.gl[rows, :] = g.astype(BF16)
        return c

    lax.fori_loop(lo, hi, tile, 0)


def stage_segments(R):
    seg = R.seg[...].astype(F32)
    cols = jnp.broadcast_to(seg, (128, R.rows)).T
    R.stats[0, :, 2:3] = cols[:, :1]
    for b in range(8):
        i, j = FORE[b]
        R.bias[BASE[b] : BASE[b + 1], :] = jnp.where(cols[i:j] == seg[:, 128 * b : 128 * b + 128], 0.0, neg_fill)


def stage_cotangent(R):
    def tile(i, c):
        rows = pl.ds(pl.multiple_of(i * TILE, TILE), TILE)
        g = jnp.where(R.stats[0, rows, 2:3] >= 0.0, R.cot[rows, :], 0.0)
        R.g[rows, :] = g
        R.gl[rows, :] = g.astype(BF16)
        return c

    lax.fori_loop(0, R.rows // TILE, tile, 0)


def compute(R, streams, hook):
    R.vacc[...] = jnp.zeros(R.vacc.shape, F32)
    stage_segments(R)
    for l in range(2):
        hook("qkv", l)
        stage_qkv(R, l, streams[l])
        hook("att", l)
        stage_attend(R, l, hook)
        hook("mlp", l)
        stage_mlp(R, l, streams[l], streams[l + 1], hook)
    hook("fwd", 0)
    stage_cotangent(R)
    for l in (1, 0):
        stage_weight_down(R, l)
        hook("dD", l)
        stage_mlp_back(R, l, hook)
        hook("b0", l)
        stage_weight_up(R, l)
        hook("dU", l)
        stage_weight_out(R, l)
        hook("dO", l)
        if l:
            stage_attend_back(R, l, hook)
            hook("pair2", l)
        else:
            for pr in range(3):
                stage_attend_back(R, l, hook, pr)
                hook("pair" + str(pr), l)
        stage_qkv_back(R, l, 0, 1)
        hook("half", l)
        stage_qkv_back(R, l, 1, 2)
        hook("b1", l)


MESH = pl.DeviceIdType.MESH
VECTORS = 8


def scratch_single(rows, d, f):
    v = pltpu.VMEM
    return dict(
        mid=v((rows, d), F32), n1=v((2, rows, d), BF16), n2=v((2, rows, d), BF16),
        stats=v((2, rows, 128), F32), aT=v((2, d, rows), BF16),
        q=v((2, rows, d), BF16), k=v((2, rows, d), BF16), v=v((2, rows, d), BF16),
        att=v((rows, d), BF16), attT=v((2, d, rows), BF16), mT=v((2, d, rows), BF16),
        hidT=v((2, f, rows), BF16), slope=v((2, rows, f), BF16),
        bias=v((BASE[8], 128), F32), lse=v((2, 3, 2, rows), F32), fb=v((SLOTS, SLOT, 256), F32),
        midb=v((TILE, d), F32),
        gl=v((rows, d), BF16), gml=v((rows, d), BF16),
        dproj=v((rows, 3 * d), BF16), vacc=v((24, 8, d), F32),
    )


def scratch_comm(d, f):
    v, dma = pltpu.VMEM, pltpu.SemaphoreType.DMA
    s, t = d // 8, f // 8
    return dict(
        wqkv=v((2, d, 3 * d), BF16), wo=v((2, d, d), BF16), wup=v((2, d, f), BF16), wd=v((2, f, d), BF16),
        pk=v((24, 128), F32), mine=v((24, d), BF16), gat=v((8, 24, d), BF16), vec=v((24, d), F32),
        dD=v((2, 4, t, d), BF16), dU=v((2, 4, s, f), BF16), dA=v((4, 2, 4, s, d), BF16),
        pD=v((2, 4, t, d), BF16), pU=v((2, 4, s, f), BF16), pA=v((8, 4, s, d), BF16),
        xD=v((2, 3, t, d), BF16), xU=v((2, 3, s, f), BF16), xA=v((8, 3, s, d), BF16),
        zb=v((4, 4, s, d), BF16), zr=v((4, 3, s, d), BF16), zs=v((4, s, d), BF16),
        yb=v((8, s, d), BF16), yr=v((8, 3, s, d), BF16), ys=v((8, s, d), BF16),
        v0=v((2, 12, d), F32), v1=v((2, 12, d), F32), v2=v((2, 12, d), F32), v3=v((2, 3, 12, d), F32), v4=v((2, 4, 12, d), F32),
        vs=v((2, 12, d), F32), vl=dma((2,)), loc=dma((9,)), ags=dma((9,)), agr=dma((9, 3)),
        s1s=dma((14,)), s1r=dma((14,)), s2s=dma((14,)), s2r=dma((14,)), s3s=dma((14,)), s3r=dma((14,)), s4s=dma((12,)), s4r=dma((12,)),
    )


OWNER = (0, 3, 1, 2)


class Comm:
    def __init__(self, R):
        self.R = R
        self.f = lax.axis_index("fsdp")
        self.z = lax.axis_index("rep")
        f = self.f
        self.c = lax.rem(f, 2)
        self.p = f // 2
        dx = 1 - 2 * lax.rem(self.p, 2)
        dy = 2 - 4 * (self.p // 2)
        self.chip = (self.p, self.p + dx, self.p + dy, self.p + dx + dy)
        self.core = 1 - self.c
        self.partner = self.dev(self.p, self.core)
        self.steps = (
            self.own, self.relay, self.diagonal, self.have, self.step1, self.step2, self.step3, self.step4, self.step5,
            self.vec1, self.vec2, self.vec3, self.vec4)

    def dev(self, chip, core):
        return {"fsdp": 2 * chip + core}

    def rep(self, d):
        return lax.rem(self.z + d, 4)

    def push(self, src, dst, ss, rs, dev):
        pltpu.make_async_remote_copy(src, dst, ss, rs, device_id=dev, device_id_type=MESH).start()

    def got(self, ref, sem):
        pltpu.make_async_remote_copy(ref, ref, sem, sem, device_id=self.partner, device_id_type=MESH).wait_recv()

    def sent(self, ref, sem):
        pltpu.make_async_remote_copy(ref, ref, sem, sem, device_id=self.partner, device_id_type=MESH).wait_send()

    def barrier(self):
        bar = pltpu.get_barrier_semaphore()
        for dev in self.peers():
            pl.semaphore_signal(bar, inc=1, device_id=dev, device_id_type=MESH)
        pl.semaphore_wait(bar, 7)

    def peers(self):
        out = [self.partner]
        out += [self.dev(self.chip[k], self.c) for k in (1, 2, 3)]
        out += [{"rep": self.rep(d)} for d in (1, 2, 3)]
        return out

    def shards(self, i, f, n=1):
        R = self.R
        if i == 0:
            return R.gat.at[pl.ds(f, n)]
        l, k = (i - 1) // 4, (i - 1) % 4
        ref = (R.wqkv, R.wo, R.wup, R.wd)[k]
        m = ref.shape[1] // 8
        return ref.at[l, pl.ds(pl.multiple_of(f * m, m), n * m)]

    def half(self, i, f, h):
        R = self.R
        l, k = (i - 1) // 4, (i - 1) % 4
        ref = (R.wqkv, R.wo, R.wup, R.wd)[k]
        m, w = ref.shape[1] // 8, ref.shape[2]
        cut = w // 256 * 128
        return ref.at[l, pl.ds(pl.multiple_of(f * m, m), m), pl.ds(0, cut) if h == 0 else pl.ds(cut, w - cut)]

    def source(self, i):
        R = self.R
        if i == 0:
            return R.mine
        l, k = (i - 1) // 4, (i - 1) % 4
        return (R.sqkv, R.so, R.sup, R.sd)[k].at[l]

    def target(self, i):
        return self.R.gat.at[self.f] if i == 0 else self.shards(i, self.f)

    def own(self, i):
        R, src, dst = self.R, self.source(i), self.target(i)
        for k in (1, 2, 3) if i < 2 else (1, 2):
            self.push(src, dst, R.ags.at[i], R.agr.at[i, 0], self.dev(self.chip[k], self.c))
        self.push(src, dst, R.ags.at[i], R.agr.at[i, 2], self.partner)
        pltpu.make_async_copy(src, dst, R.loc.at[i]).start()

    def forward(self, i, k):
        here = self.shards(i, 2 * self.chip[k] + self.c)
        self.push(here, here, self.R.ags.at[i], self.R.agr.at[i, 2], self.partner)

    def relay(self, i):
        R = self.R
        self.got(self.shards(i, 0, 3 if i < 2 else 2), R.agr.at[i, 0])
        if i >= 2:
            for h, (src, to) in enumerate(((1, 2), (2, 1))):
                here = self.half(i, 2 * self.chip[src] + self.c, h)
                self.push(here, here, R.ags.at[i], R.agr.at[i, 1], self.dev(self.chip[to], self.c))
        for k in (1, 2, 3) if i < 2 else (1, 2):
            self.forward(i, k)

    def diagonal(self, i):
        self.got(self.shards(i, 0), self.R.agr.at[i, 1])
        self.forward(i, 3)

    def have(self, i):
        R = self.R
        pltpu.make_async_copy(self.source(i), self.target(i), R.loc.at[i]).wait()
        self.got(self.shards(i, 0, 4), R.agr.at[i, 2])

    def grads(self, t):
        R = self.R
        if t < 4:
            l = t // 2
            d, p, x = ((R.dD, R.pD, R.xD), (R.dU, R.pU, R.xU))[t % 2]
            return d, p.at[l], x.at[l]
        return R.dA.at[t % 4], R.pA.at[t - 4], R.xA.at[t - 4]

    def step1(self, t):
        R = self.R
        d, p, x = self.grads(t)
        self.push(d.at[self.core], p, R.s1s.at[t], R.s1r.at[t], self.partner)

    def step2(self, t):
        R = self.R
        d, p, x = self.grads(t)
        self.sent(d.at[self.core], R.s1s.at[t])
        self.got(p, R.s1r.at[t])
        for k in (3, 1, 2, 0):
            ch = self.chip[k]
            p[ch] = (d[self.c, ch].astype(F32) + p[ch].astype(F32)).astype(BF16)
            if k:
                self.push(p.at[ch], x.at[k - 1], R.s2s.at[t], R.s2r.at[t], self.dev(ch, self.c))

    def step3(self, t):
        R = self.R
        d, p, x = self.grads(t)
        self.got(x, R.s2r.at[t])
        self.sent(x, R.s2s.at[t])

        def total(*at):
            tot = p[(self.p, *at)].astype(F32)
            for k in range(3):
                tot = tot + x[(k, *at)].astype(F32)
            return tot.astype(BF16)

        s, w = R.zb.shape[2:]
        if t >= 4:
            u, owner = t - 4, OWNER[t % 4]
            R.yb[u] = total(slice(None), slice(None))

            @pl.when(self.z != owner)
            def _():
                slot = lax.rem(self.z + 3 - owner, 4)
                self.push(R.yb.at[u], R.yr.at[u, slot], R.s3s.at[t], R.s3r.at[t], {"rep": owner})

            return
        for j in range(4):
            rows, cols = slice(s * j, s * j + s), slice(w * j, w * j + w)
            R.zb[t, j] = total(rows, slice(None)) if t % 2 == 0 else total(slice(None), cols)
        for e in (1, 2, 3):
            r = self.rep(e)
            self.push(R.zb.at[t, r], R.zr.at[t, e - 1], R.s3s.at[t], R.s3r.at[t], {"rep": r})

    def place(self, t):
        return (t % 2 + 3 * (t // 2), None) if t < 4 else (3 * ((t - 4) // 4) + 2, t % 4)

    def step4(self, t):
        R = self.R
        row, j = self.place(t)
        if t >= 4:
            u, owner = t - 4, OWNER[t % 4]

            @pl.when(self.z == owner)
            def _():
                self.got(R.yr.at[u], R.s3r.at[t])
                tot = R.yb[u].astype(F32)
                for k in range(3):
                    tot = tot + R.yr[u, k].astype(F32)
                R.ys[u] = tot.astype(BF16)
                here = R.zout.at[row, j]
                for e in (1, 2, 3):
                    self.push(R.ys.at[u], here, R.s4s.at[t], R.s4r.at[t], {"rep": (owner + e) % 4})
                pltpu.make_async_copy(R.ys.at[u], here, R.s4r.at[t]).start()

            return
        self.got(R.zr.at[t], R.s3r.at[t])
        self.sent(R.zr.at[t], R.s3s.at[t])
        tot = R.zb[t, self.z].astype(F32)
        for k in range(3):
            tot = tot + R.zr[t, k].astype(F32)
        R.zs[t] = tot.astype(BF16)
        here = R.zout.at[row, self.z]
        for e in (1, 2, 3):
            self.push(R.zs.at[t], here, R.s4s.at[t], R.s4r.at[t], {"rep": self.rep(e)})
        pltpu.make_async_copy(R.zs.at[t], here, R.s4r.at[t]).start()

    def step5(self, t):
        R = self.R
        row, j = self.place(t)
        if t >= 4:
            u, owner = t - 4, OWNER[t % 4]
            self.got(R.zout.at[row, j], R.s4r.at[t])

            @pl.when(self.z == owner)
            def _():
                self.sent(R.yr.at[u], R.s4s.at[t])

            @pl.when(self.z != owner)
            def _():
                self.sent(R.yb.at[u], R.s3s.at[t])

            return
        self.got(R.zout.at[row], R.s4r.at[t])
        self.sent(R.zr.at[t], R.s4s.at[t])

    def vec1(self, l):
        R, t = self.R, 12 + l
        R.v0[l] = jnp.sum(R.vacc[12 * l : 12 * l + 12], axis=1)
        self.push(R.v0.at[l], R.v1.at[l], R.s1s.at[t], R.s1r.at[t], self.partner)

    def vec2(self, l):
        R, t = self.R, 12 + l
        self.got(R.v1.at[l], R.s1r.at[t])
        self.sent(R.v0.at[l], R.s1s.at[t])
        R.v2[l] = R.v0[l] + R.v1[l]
        for k in (1, 2, 3):
            self.push(R.v2.at[l], R.v3.at[l, k - 1], R.s2s.at[t], R.s2r.at[t], self.dev(self.chip[k], self.c))

    def vec3(self, l):
        R, t = self.R, 12 + l
        self.got(R.v3.at[l], R.s2r.at[t])
        self.sent(R.v3.at[l], R.s2s.at[t])
        tot = R.v2[l]
        for k in (1, 2, 3):
            tot = tot + R.v3[l, k - 1]
        R.v4[l, self.z] = tot
        here = R.v4.at[l, self.z]
        for e in (1, 2, 3):
            self.push(here, here, R.s3s.at[t], R.s3r.at[t], {"rep": self.rep(e)})

    def vec4(self, l):
        R, t = self.R, 12 + l
        self.got(R.v3.at[l], R.s3r.at[t])
        self.sent(R.v3.at[l], R.s3s.at[t])
        R.vs[l] = (R.v4[l, 0] + R.v4[l, 1]) + (R.v4[l, 2] + R.v4[l, 3])
        pltpu.make_async_copy(R.vs.at[l], R.vout.at[l], R.vl.at[l]).start()

    def late_sends(self):
        for i in range(9):
            self.sent(self.shards(i, 0, 7), self.R.ags.at[i])

    def late_io(self, save):
        R = self.R
        pltpu.make_async_copy(R.xb, R.out, R.io.at[1]).wait()
        save.wait()
        for l in range(2):
            pltpu.make_async_copy(R.vs.at[l], R.vout.at[l], R.vl.at[l]).wait()

    def place_vectors(self):
        R = self.R
        R.pk[...] = jnp.zeros(R.pk.shape, F32)
        n = R.small[0].shape[1]
        for l in range(2):
            for k, ref in enumerate(R.small[:8]):
                R.pk[12 * l + k : 12 * l + k + 1, :n] = ref[l : l + 1, :].astype(F32)
        row = lax.broadcasted_iota(jnp.int32, (128, 384), 0)
        col = lax.broadcasted_iota(jnp.int32, (128, 384), 1)
        put = (col == row + n * self.f) & (row < n)
        R.mine[...] = nn(R.pk[...].astype(BF16), put.astype(F32).astype(BF16)).astype(BF16)
        ub = R.small[8]
        w = ub.shape[1]
        row = lax.broadcasted_iota(jnp.int32, (w, 384), 0)
        col = lax.broadcasted_iota(jnp.int32, (w, 384), 1)
        put = (col == row + w * lax.rem(self.f, 2)).astype(F32).astype(BF16)
        moved = nn(ub[...], put)
        for l in range(2):
            for h in range(4):
                R.mine[12 * l + 8 + h : 12 * l + 9 + h, :] = (moved[l : l + 1, :] * (self.p == h).astype(F32)).astype(BF16)


def single_kernel(names, *refs):
    R = NS(**dict(zip(names, refs)))
    R.rows = R.x.shape[0]
    R.datt, R.g = R.att, R.gin
    R.dk, R.dv = R.dkv.at[0], R.dkv.at[1]
    R.grad = lambda k, l: (R.dD, R.dU, R.dA)[k].at[l]
    compute(R, (R.x, R.mid, R.out), lambda *a: None)
    R.vg[...] = jnp.sum(R.vacc[...], axis=1)


def single(x, cot, seg, vec, wqkv, wo, wup, wd):
    (rows, d), f = x.shape, wd.shape[1]
    sc = dict(dkv=pltpu.VMEM((2, rows, 128), F32), **scratch_single(rows, d, f))
    names = ("x", "cot", "seg", "vec", "wqkv", "wo", "wup", "wd", "out", "gin", "dA", "dU", "dD", "vg", *sc)
    s = jax.ShapeDtypeStruct
    return pl.pallas_call(
        functools.partial(single_kernel, names),
        out_shape=(
            s((rows, d), F32), s((rows, d), F32), s((2, 4, 2, 4, d // 8, d), BF16), s((2, 2, 4, d // 8, f), BF16),
            s((2, 2, 4, f // 8, d), BF16), s((24, d), F32)),
        in_specs=[pl.BlockSpec(memory_space=pltpu.VMEM)] * 8,
        out_specs=[pl.BlockSpec(memory_space=pltpu.VMEM)] * 6,
        scratch_shapes=list(sc.values()),
        compiler_params=pltpu.CompilerParams(vmem_limit_bytes=67043328),
    )(x, cot, seg, vec, wqkv, wo, wup, wd)


OWN, RELAY, DIAG, HAVE, S1, S2, S3, S4, S5, V1, V2, V3, V4 = range(13)
PLAN = {
    ("start", 0): ((OWN, 0), (OWN, 1), (OWN, 2), (OWN, 3), (OWN, 4),),
    ("qkv", 0): ((RELAY, 0), (RELAY, 1), (HAVE, 0), (HAVE, 1),),
    ("att", 0): ((RELAY, 2),),
    ("att1", 0): ((RELAY, 3), (RELAY, 4), (OWN, 5),),
    ("att2", 0): ((DIAG, 2), (DIAG, 3), (OWN, 6),),
    ("mlp", 0): ((DIAG, 4), (HAVE, 2), (HAVE, 3), (HAVE, 4),),
    ("mlp1", 0): ((RELAY, 5), (OWN, 7),),
    ("mlp2", 0): ((RELAY, 6),),
    ("mlp3", 0): ((DIAG, 5), (OWN, 8),),
    ("qkv", 1): ((HAVE, 5),),
    ("att", 1): ((RELAY, 7), (DIAG, 6),),
    ("att1", 1): ((RELAY, 8),),
    ("att2", 1): ((DIAG, 7),),
    ("mlp", 1): ((DIAG, 8), (HAVE, 6), (HAVE, 7), (HAVE, 8),),
    ("dD", 1): ((S1, 2),),
    ("b0t1", 1): ((S2, 2),),
    ("dU", 1): ((S1, 3),),
    ("dO", 1): ((S1, 11),),
    ("pr1", 1): ((S3, 2), (S2, 3), (S2, 11), (S1, 8),),
    ("pr2", 1): ((S2, 8), (S1, 9),),
    ("pair2", 1): ((S4, 2), (S2, 9), (S1, 10),),
    ("half", 1): ((S2, 10),),
    ("b1", 1): ((V1, 1),),
    ("dD", 0): ((S1, 0), (V2, 1), (S3, 3),),
    ("b0t1", 0): ((S3, 11),),
    ("b0t2", 0): ((S2, 0), (S3, 8),),
    ("b0t3", 0): ((S4, 3), (S3, 9),),
    ("b0", 0): ((S3, 10), (S4, 11),),
    ("dU", 0): ((S1, 1), (V3, 1), (S4, 8),),
    ("dO", 0): ((S1, 7), (S4, 9), (S2, 1), (S3, 0),),
    ("pair0", 0): ((S2, 7), (S1, 4), (S4, 10),),
    ("pair1", 0): ((S2, 4), (S1, 5), (V4, 1),),
    ("pair2", 0): ((S3, 1), (S2, 5), (S1, 6), (S4, 0),),
    ("half", 0): ((S3, 7), (S2, 6),),
    ("b1", 0): ((V1, 0), (S3, 4),),
    ("tail", 0): ((V2, 0), (S3, 5), (S3, 6), (V3, 0), (S4, 1), (S4, 7), (S4, 4), (S4, 5), (S4, 6), (V4, 0), (S5, 2), (S5, 3), (S5, 8), (S5, 9), (S5, 10), (S5, 11), (S5, 0), (S5, 7), (S5, 1), (S5, 4), (S5, 5), (S5, 6),),
}


def fused_kernel(names, *refs):
    R = NS(**dict(zip(names, refs)))
    R.small = [getattr(R, "p%d" % i) for i in range(9)]
    R.rows = R.xb.shape[0]
    R.datt, R.g = R.att, R.mid
    R.dk, R.dv = R.cot.at[:, :128], R.cot.at[:, 128:256]
    R.grad = lambda k, l: (R.dD, R.dU, R.dA)[k]
    load = pltpu.make_async_copy(R.x, R.xb, R.io.at[0])
    load.start()
    cot = pltpu.make_async_copy(R.hcot, R.cot, R.io.at[3])
    cot.start()
    C = Comm(R)
    C.place_vectors()
    C.barrier()

    def hook(name, l):
        for item in PLAN.get((name, l), ()):
            C.steps[item[0]](item[1])
        if (name, l) == ("qkv", 0):
            R.vec[...] = jnp.sum(R.gat[...].astype(F32), axis=0)
        if name == "fwd":
            pltpu.make_async_copy(R.xb, R.out, R.io.at[1]).start()
            cot.wait()

    hook("start", 0)
    load.wait()
    compute(R, (R.xb, R.mid, R.xb), hook)
    save = pltpu.make_async_copy(R.g, R.gin, R.io.at[2])
    save.start()
    hook("tail", 0)
    C.late_sends()
    C.late_io(save)


def fused(x, cot, seg, small, sqkv, so, sup, sd):
    (rows, d), f = x.shape, 8 * sd.shape[1]
    sc = dict(xb=pltpu.VMEM((rows, d), F32), cot=pltpu.VMEM((rows, d), F32), io=pltpu.SemaphoreType.DMA((4,)), **scratch_single(rows, d, f), **scratch_comm(d, f))
    ins = ("x", "hcot", "seg", *("p%d" % i for i in range(9)), "sqkv", "so", "sup", "sd")
    names = (*ins, "out", "gin", "zout", "vout", *sc)
    s = jax.ShapeDtypeStruct
    any_, vm = pl.BlockSpec(memory_space=pl.ANY), pl.BlockSpec(memory_space=pltpu.VMEM)
    return pl.pallas_call(
        functools.partial(fused_kernel, names),
        out_shape=(s((rows, d), F32), s((rows, d), F32), s((6, 4, d // 8, d), BF16), s((2, 12, d), F32)),
        in_specs=[any_] * 2 + [vm] * 10 + [any_] * 4,
        out_specs=[any_] * 4,
        scratch_shapes=list(sc.values()),
        compiler_params=pltpu.CompilerParams(vmem_limit_bytes=67043328, collective_id=0, has_side_effects=True),
    )(x, cot, seg, *small, sqkv, so, sup, sd)


def finish_kernel(*refs):
    ins, outs = refs[:4], refs[4:19]
    zb, vb, buf, sem = refs[-4:]
    vals = refs[19:-4]
    rows = buf.shape[1]
    load = [pltpu.make_async_copy(ins[i], dst, sem.at[i]) for i, dst in ((2, zb), (3, vb), (0, buf.at[0]), (1, buf.at[1]))]
    for cp in load:
        cp.start()
    save = [pltpu.make_async_copy(src, dst, sem.at[4 + i]) for i, (src, dst) in enumerate(zip((buf.at[0], buf.at[1], *vals), outs))]
    n1g, n1b, qkv, qb, vbias, wo, ob, n2g, n2b, up, ub, down, db = vals
    f = lax.axis_index("fsdp")
    s, w = zb.shape[2:]
    load[0].wait()
    for l in range(2):
        for j in range(4):
            up[l, :, w * j : w * j + w] = zb[3 * l + 1, j].astype(F32)
    save[11].start()
    for l in range(2):
        for j in range(4):
            down[l, s * j : s * j + s, :] = zb[3 * l, j].astype(F32)
    save[13].start()
    for l in range(2):
        for j in range(3):
            for k in range(3):
                qkv[l, :, w * k + 128 * j : w * k + 128 * j + 128] = zb[3 * l + 2, j, :, 128 * k : 128 * k + 128].astype(F32)
        wo[l] = zb[3 * l + 2, 3].astype(F32)
    save[4].start()
    save[7].start()
    for i in (0, 1):
        load[2 + i].wait()
        save[i].start()
    load[1].wait()
    shift = lax.rem(w - 4 * s * lax.rem(f, 2), w)
    for l in range(2):
        v = pltpu.roll(vb[l], lax.rem(w - s * f, w), 1)
        for k, ref in enumerate((n1g, n1b, qb, vbias, ob, n2g, n2b, db)):
            ref[l : l + 1, :] = v[k : k + 1, :s]
        row = vb[l, pl.ds(8 + f // 2, 1), :]
        ub[l : l + 1, :] = pltpu.roll(jnp.broadcast_to(row, (8, w)), shift, 1)[:1, : 4 * s]
    for i in (2, 3, 5, 6, 8, 9, 10, 12, 14):
        save[i].start()
    for cp in save:
        cp.wait()


def finish(out, gin, zout, vout):
    rows, d = out.shape
    s = d // 8
    shapes = ((2, s), (2, s), (2, s, 3 * d), (2, s), (2, s), (2, s, d), (2, s), (2, s), (2, s), (2, s, 4 * d), (2, 4 * s), (2, 4 * s, d), (2, s))
    any_ = pl.BlockSpec(memory_space=pl.ANY)
    return pl.pallas_call(
        finish_kernel,
        out_shape=[jax.ShapeDtypeStruct(t, F32) for t in ((rows, d), (rows, d), *shapes)],
        in_specs=[any_] * 4,
        out_specs=[any_] * 15,
        scratch_shapes=[pltpu.VMEM(t, F32) for t in shapes]
        + [pltpu.VMEM(zout.shape, BF16), pltpu.VMEM(vout.shape, F32), pltpu.VMEM((2, rows, d), F32), pltpu.SemaphoreType.DMA((19,))],
    )(out, gin, zout, vout)


def local_fused(x, cot, seg, n1g, n1b, qkv, qb, vb, wo, ob, n2g, n2b, up, ub, down, db):
    small = (n1g, n1b, qb, vb, ob, n2g, n2b, db, ub)
    return finish(*fused(x, cot, seg[None], small, qkv, wo, up, down))


def local_plain(x, cot, seg, n1g, n1b, qkv, qb, vb, wo, ob, n2g, n2b, up, ub, down, db):
    def gather(a):
        return lax.all_gather(a, "fsdp", axis=1, tiled=True)

    def scatter(a):
        return lax.psum(lax.psum_scatter(a, "fsdp", scatter_dimension=1, tiled=True), "rep")

    d = x.shape[1]
    vecs = jnp.stack([gather(a) for a in (n1g, n1b, qb, vb, ob, n2g, n2b, db)], 1)
    vec = jnp.concatenate([vecs, gather(ub).reshape(2, 4, d)], 1).astype(F32).reshape(24, d)
    out, gin, da, du, dd, vg = single(x, cot, seg[None], vec, gather(qkv), gather(wo), gather(up), gather(down))
    du, dd = (jnp.swapaxes(a, 1, 2).reshape(2, -1, a.shape[-1]).astype(F32) for a in (du, dd))
    da = jnp.transpose(da, (0, 3, 2, 4, 1, 5)).reshape(2, d, 4, d).astype(F32)
    dqkv = jnp.swapaxes(da[:, :, :3].reshape(2, d, 3, 3, d // 3), 2, 3).reshape(2, d, 3 * d)
    dqkv, dwo, du, dd = scatter(dqkv), scatter(da[:, :, 3]), scatter(du), scatter(dd)
    vg = vg.reshape(2, 12, d)
    g = [scatter(vg[:, k]) for k in range(8)]
    gub = scatter(vg[:, 8:].reshape(2, 4 * d))
    return (out, gin, g[0], g[1], dqkv, g[2], g[3], dwo, g[4], g[5], g[6], du, gub, dd, g[7])


def solution(mesh):
    from jax.sharding import PartitionSpec as P

    vec, mat, row = P(None, "fsdp"), P(None, "fsdp", None), P(("rep", "fsdp"), None)
    params = (vec, vec, mat, vec, vec, mat, vec, vec, vec, mat, vec, mat, vec)
    local = local_fused if dict(mesh.shape) == {"rep": 4, "fsdp": 8} else local_plain
    return jax.shard_map(local, mesh=mesh, in_specs=(row, row, P(("rep", "fsdp")), *params), out_specs=(row, row, *params), check_vma=False)
```
